512 devices in a mesh: layer: 4 (over z_lo), row: 8 (over z_hi, core), col: 16 (over y, x).
Axes of the slice: x: 4, y: 4, z: 16 (z_hi: 4, z_lo: 4; z = z_hi * 4 + z_lo), core: 2. Of those that a mesh axis runs over, the one named last changes fastest.
Arguments:
- panels: float32 [16384, 8192], P('row', ('layer', 'col')), may hold values from -0.0625 to 0.0625
- eigvecs: float32 [8192, 2048], P(('layer', 'row'), 'col'), may hold values from -6 to 6
Outputs:
- result: float32 [16384, 2048], P('row', 'col')
The draws below stay inside these ranges and needn't reach their ends.
All inputs are finite; a program needn't handle non-finite values.
Results may differ from the reference program's by a relative error of at most 0.0001.
Values sent between devices are 32-bit elements; how exact they have to be, the bound alone decides.
A program may use at most 64 MiB of HBM per device.

```python
import jax
import jax.numpy as jnp
from jax import lax

NB = 1024
PANELS = 2
NEV = 2048
ROWS = 16384
INNER = 8192
N_LAYER = 4


def block_scale(stream_key, dims, shards, least, largest):
    loudness, own = 1.0, jax.random.fold_in(stream_key, 6)
    for axis_at, blocks in shards:
        draws = jnp.exp(jax.random.uniform(jax.random.fold_in(own, axis_at), (blocks,), jnp.float32, least / len(shards), largest / len(shards)))
        loudness = loudness * jnp.repeat(draws, dims[axis_at] // blocks).reshape([-1 if axis == axis_at else 1 for axis in range(len(dims))])
    return loudness


def bell_draw(own_key, dims, deviation, bound, pieces=(), dtype=jnp.bfloat16):
    level = block_scale(own_key, dims, pieces, -0.22, 0.18) if pieces else 1.0
    entries = jax.random.normal(own_key, dims, jnp.float32) * deviation * level
    return jnp.minimum(jnp.maximum(entries, -bound), bound).astype(dtype)


def setup_inputs(seed: int = 0) -> dict:
    arg_keys = jax.random.split(jax.random.key(seed), 3)
    return {
        "panels": bell_draw(arg_keys[0], (ROWS, INNER), INNER ** -0.5, 0.0625, ((0, 8), (1, 64)), jnp.float32),
        "eigvecs": bell_draw(arg_keys[1], (INNER, NEV), 1.0, 6.0, ((0, 32), (1, 16)), jnp.float32),
    }


def reference(panels, eigvecs):
    group = PANELS * NB
    result = jnp.zeros((panels.shape[0], eigvecs.shape[1]), jnp.float32)
    for index in range(N_LAYER):
        partial_value = jnp.dot(panels[:, index * group:(index + 1) * group], eigvecs[index * group:(index + 1) * group, :], preferred_element_type=jnp.float32, precision=lax.Precision.HIGHEST)
        result = result + partial_value
    return result
```

```python
import jax
import jax.numpy as jnp
from jax import lax
from jax.experimental import pallas as pl
from jax.experimental.pallas import tpu as pltpu
from jax.sharding import PartitionSpec as P

MESH = pl.DeviceIdType.MESH
CHUNKS = 8
BK = 128


def remote(src, dst, send, recv, device):
    return pltpu.make_async_remote_copy(src_ref=src, dst_ref=dst, send_sem=send, recv_sem=recv, device_id=device, device_id_type=MESH)


def drain(ref, sem):
    pltpu.make_async_copy(ref, ref, sem).wait()


def halves(x):
    hi = x.astype(jnp.bfloat16)
    return hi, (x - hi.astype(jnp.float32)).astype(jnp.bfloat16)


def kernel(
    a_ref, e_ref, o_ref,
    a_low, a_high, a_far, b_first, b_second, b_far, b_all, b_cat, prod,
    half_up, half_down, sum_up, sum_down, z_mine, z_in, z_pair, z_other,
    as_up, as_down, ar_low, ar_high, as_far, ar_far,
    bs_first, br_first, bs_second, br_second, bs_far, br_far, bs_plane, br_plane,
    ps_half, pr_up, pr_down, ps_up, ps_down, qr_up, qr_down,
    zs_in, zr_in, zs_pair, zr_pair, zs_out, zr_out,
):
    layer, row, col = lax.axis_index("layer"), lax.axis_index("row"), lax.axis_index("col")
    zh, core = lax.div(row, 2), lax.rem(row, 2)
    y, x = lax.div(col, 4), lax.rem(col, 4)
    ga = x + core * (y - x)
    gb = y + core * (x - y)

    def at(a, b):
        return {"col": (1 - core) * (b * 4 + a) + core * (a * 4 + b)}

    a_up, a_down = at(lax.rem(ga + 1, 4), gb), at(lax.rem(ga + 3, 4), gb)
    b_up, b_down = at(ga, lax.rem(gb + 1, 4)), at(ga, lax.rem(gb + 3, 4))
    step = 1 - 2 * core
    zh_first, zh_second = lax.rem(zh + step + 4, 4), lax.rem(zh - step + 4, 4)
    z_first, z_second = {"row": zh_first * 2 + core}, {"row": zh_second * 2 + core}
    outer = jnp.logical_or(layer == 0, layer == 3)
    inner = jnp.logical_not(outer)
    z_inner = {"layer": 1 + lax.div(layer, 2)}
    z_partner = {"layer": lax.rem(3 - layer, 4)}
    z_outer = {"layer": lax.rem(3 * layer + 1, 4)}

    barrier = pltpu.get_barrier_semaphore()

    def greet(device):
        pl.semaphore_signal(barrier, inc=1, device_id=device, device_id_type=MESH)

    for device in (a_up, a_down, b_up, b_down, z_first, z_second):
        greet(device)

    @pl.when(outer)
    def _():
        greet(z_inner)

    @pl.when(inner)
    def _():
        greet(z_partner)
        greet(z_outer)

    @pl.when(core == 0)
    def _():
        for yy in range(4):
            greet({"row": zh * 2 + 1, "col": yy * 4 + x})
        for d in range(1, 4):
            greet({"row": zh * 2, "col": lax.rem(y + d, 4) * 4 + x})

    @pl.when(core == 1)
    def _():
        for d in range(1, 4):
            greet({"row": zh * 2 + lax.div(x, 2), "col": y * 4 + lax.rem(x + d, 4)})

        @pl.when(x < 2)
        def _():
            greet({"row": zh * 2})

    pl.semaphore_wait(barrier, 6 + (2 - outer.astype(jnp.int32)) + 3 + core + 2 - core * lax.div(x, 2))

    firsts = [remote(e_ref.at[h], b_first.at[h], bs_first.at[h], br_first.at[h], z_first) for h in range(2)]
    seconds = [remote(e_ref.at[h], b_second.at[h], bs_second.at[h], br_second.at[h], z_second) for h in range(2)]
    b_fars = [remote(b_first.at[h], b_far.at[h], bs_far.at[h], br_far.at[h], z_first) for h in range(2)]
    half = a_ref.shape[0] // 2
    rows = [pl.ds(h * half, half) for h in range(2)]
    ups = [remote(a_ref.at[rows[h]], a_low.at[rows[h]], as_up.at[h], ar_low.at[h], a_up) for h in range(2)]
    downs = [remote(a_ref.at[rows[h]], a_high.at[rows[h]], as_down.at[h], ar_high.at[h], a_down) for h in range(2)]
    far_up = remote(a_low.at[rows[0]], a_far.at[rows[0]], as_far.at[0], ar_far.at[0], a_up)
    far_down = remote(a_high.at[rows[1]], a_far.at[rows[1]], as_far.at[1], ar_far.at[1], a_down)

    for c in firsts:
        c.start()
    ups[0].start()
    downs[1].start()
    ups[1].start()
    downs[0].start()

    ends = []

    def either(own, copy, local):
        @pl.when(own)
        def _():
            local.start()

        @pl.when(jnp.logical_not(own))
        def _():
            copy.start()

        def end():
            @pl.when(jnp.logical_not(own))
            def _():
                copy.wait_send()

        ends.append(end)

    def in_plane(src, source, k):
        dst = b_all.at[pl.ds(2 * core, 2), y]
        either(
            jnp.logical_and(core == 0, source == y),
            remote(src, dst, bs_plane.at[3 * k], br_plane.at[y], {"row": zh * 2, "col": source * 4 + x}),
            pltpu.make_async_copy(src, dst, br_plane.at[y]),
        )
        for q in range(2):
            dst = b_all.at[source, x]
            either(
                jnp.logical_and(core == 1, x == 2 * core + q),
                remote(src.at[q], dst, bs_plane.at[3 * k + 1 + q], br_plane.at[x], {"row": zh * 2 + 1, "col": y * 4 + 2 * core + q}),
                pltpu.make_async_copy(src.at[q], dst, br_plane.at[x]),
            )

    in_plane(e_ref, zh, 0)
    for h in range(2):
        firsts[h].wait_recv()
        b_fars[h].start()
        seconds[h].start()
    in_plane(b_first, zh_second, 1)
    ups[0].wait_recv()
    far_up.start()
    downs[1].wait_recv()
    far_down.start()
    for h in range(2):
        seconds[h].wait_recv()
    in_plane(b_second, zh_first, 2)
    for h in range(2):
        b_fars[h].wait_recv()
    in_plane(b_far, lax.rem(zh + 2, 4), 3)

    for j in range(4):
        n = lax.rem(gb + j, 4)
        drain(b_all.at[:, n], br_plane.at[n])
        for i in range(4):
            hi, lo = halves(b_all[lax.rem(ga + i, 4), n])
            cols = pl.ds(j * BK, BK)
            b_cat[pl.ds(i * BK, BK), cols] = hi
            b_cat[pl.ds(512 + i * BK, BK), cols] = lo
            b_cat[pl.ds(1024 + i * BK, BK), cols] = hi
    ups[1].wait_recv()
    downs[0].wait_recv()
    far_up.wait_recv()
    far_down.wait_recv()

    size = a_ref.shape[0] // CHUNKS
    part = size // 2

    def span(m):
        return pl.ds(pl.multiple_of(m * size, size), size)

    def top(m):
        return pl.ds(pl.multiple_of(m * size, part), part)

    def bottom(m):
        return pl.ds(pl.multiple_of(m * size + part, part), part)

    def multiply(m):
        parts = [halves(ref[span(m), :]) for ref in (a_ref, a_high, a_far, a_low)]
        his, los = [p[0] for p in parts], [p[1] for p in parts]
        left = jnp.concatenate(his + his + los, axis=1)
        out = jnp.dot(left, b_cat[...], preferred_element_type=jnp.float32)
        for j in range(4):
            prod[j, span(m), :] = out[:, j * BK:(j + 1) * BK]
        remote(prod.at[2, top(m)], half_up.at[m], ps_half, pr_up.at[m], b_up).start()
        remote(prod.at[2, bottom(m)], half_down.at[m], ps_half, pr_down.at[m], b_down).start()
        remote(prod.at[1, bottom(m)], sum_up.at[bottom(m)], ps_up, qr_up.at[m], b_up).start()
        remote(prod.at[3, top(m)], sum_down.at[top(m)], ps_down, qr_down.at[m], b_down).start()

    def pass_on(m):
        drain(half_up.at[m], pr_up.at[m])
        prod[1, top(m), :] += half_up[m]
        remote(prod.at[1, top(m)], sum_up.at[top(m)], ps_up, qr_up.at[m], b_up).start()
        drain(half_down.at[m], pr_down.at[m])
        prod[3, bottom(m), :] += half_down[m]
        remote(prod.at[3, bottom(m)], sum_down.at[bottom(m)], ps_down, qr_down.at[m], b_down).start()

    def close_layer(m):
        drain(sum_up.at[span(m)], qr_up.at[m])
        drain(sum_down.at[span(m)], qr_down.at[m])
        z_mine[span(m), :] = prod[0, span(m), :] + (sum_up[span(m), :] + sum_down[span(m), :])

        @pl.when(outer)
        def _():
            remote(z_mine.at[span(m)], z_in.at[span(m)], zs_in, zr_in.at[m], z_inner).start()

    def pair_up(m):
        drain(z_in.at[span(m)], zr_in.at[m])
        z_pair[span(m), :] = z_mine[span(m), :] + z_in[span(m), :]
        remote(z_pair.at[span(m)], z_other.at[span(m)], zs_pair, zr_pair.at[m], z_partner).start()

    def finish(m):
        drain(z_other.at[span(m)], zr_pair.at[m])
        o_ref[span(m), :] = z_pair[span(m), :] + z_other[span(m), :]
        remote(o_ref.at[span(m)], o_ref.at[span(m)], zs_out, zr_out.at[m], z_outer).start()

    lags = (0, 1, 2, 4, 6)

    def body(t, carry):
        for stage, lag, cond in ((multiply, 0, None), (pass_on, 1, None), (close_layer, 2, None), (pair_up, 4, inner), (finish, 6, inner)):
            m = t - lag
            ok = jnp.logical_and(m >= 0, m < CHUNKS)
            if cond is not None:
                ok = jnp.logical_and(ok, cond)
            pl.when(ok)(lambda stage=stage, m=m: stage(m))
        return carry

    lax.fori_loop(0, CHUNKS + lags[-1], body, 0)

    @pl.when(outer)
    def _():
        for m in range(CHUNKS):
            rows_m = pl.ds(m * size, size)
            drain(o_ref.at[rows_m], zr_out.at[m])
        drain(z_mine, zs_in)

    @pl.when(inner)
    def _():
        drain(z_pair, zs_pair)
        drain(o_ref, zs_out)

    drain(prod.at[2], ps_half)
    drain(prod.at[1], ps_up)
    drain(prod.at[3], ps_down)
    for c in firsts + seconds + b_fars + ups + downs + [far_up, far_down]:
        c.wait_send()
    for end in ends:
        end()


def local(panels, eigvecs):
    m, f32 = panels.shape[0], jnp.float32
    whole = pltpu.VMEM((m, BK), f32)
    block = pltpu.VMEM((2, BK, BK), f32)
    dma = pltpu.SemaphoreType.DMA
    part = pltpu.VMEM((CHUNKS, m // CHUNKS // 2, BK), f32)
    return pl.pallas_call(
        kernel,
        out_shape=jax.ShapeDtypeStruct((m, BK), f32),
        in_specs=[pl.BlockSpec(memory_space=pltpu.VMEM)] * 2,
        out_specs=pl.BlockSpec(memory_space=pltpu.VMEM),
        scratch_shapes=[
            whole, whole, whole, block, block, block,
            pltpu.VMEM((4, 4, BK, BK), f32), pltpu.VMEM((12 * BK, 4 * BK), jnp.bfloat16), pltpu.VMEM((4, m, BK), f32),
            part, part, whole, whole, whole, whole, whole, whole,
            dma((2,)), dma((2,)), dma((2,)), dma((2,)), dma((2,)), dma((2,)),
            dma((2,)), dma((2,)), dma((2,)), dma((2,)), dma((2,)), dma((2,)), dma((12,)), dma((4,)),
            dma, dma((CHUNKS,)), dma((CHUNKS,)), dma, dma, dma((CHUNKS,)), dma((CHUNKS,)),
            dma, dma((CHUNKS,)), dma, dma((CHUNKS,)), dma, dma((CHUNKS,)),
        ],
        compiler_params=pltpu.CompilerParams(collective_id=0, has_side_effects=True),
        name="panels_by_vectors",
    )(panels, eigvecs.reshape(2, BK, BK))


def solution(mesh):
    in_specs = (P("row", ("layer", "col")), P(("layer", "row"), "col"))
    return jax.shard_map(local, mesh=mesh, in_specs=in_specs, out_specs=P("row", "col"), check_vma=False)
```

```python
import jax
import jax.numpy as jnp
from jax import lax
from jax.experimental import pallas as pl
from jax.experimental.pallas import tpu as pltpu
from jax.sharding import PartitionSpec as P

MESH = pl.DeviceIdType.MESH
CHUNKS = 8
ITEMS = 2 * CHUNKS
PIECES = 4
BK = 128
HALF = BK // 2


def remote(src, dst, send, recv, device):
    return pltpu.make_async_remote_copy(src_ref=src, dst_ref=dst, send_sem=send, recv_sem=recv, device_id=device, device_id_type=MESH)


def drain(ref, sem):
    pltpu.make_async_copy(ref, ref, sem).wait()


def parts(x):
    hi = x.astype(jnp.bfloat16)
    return hi, (x - hi.astype(jnp.float32)).astype(jnp.bfloat16)


def swap(a, b):
    left = lax.broadcasted_iota(jnp.int32, a.shape, 1) < HALF
    return jnp.where(left, a, pltpu.roll(b, HALF, 1)), jnp.where(left, pltpu.roll(a, HALF, 1), b)


def kernel(
    a_hbm, e_hbm, o_hbm,
    a_ref, e_ref, a_low, a_high, a_far, b_mine, b_first, b_second, b_far, b_all, b_cat, keep,
    go_up, go_down, in_up, in_down, late_up, late_down, end_up, end_down, z_mine, z_in, z_pair, z_other, z_sum, o_ref,
    in_sems, out_sem, as_up, as_down, ar_low, ar_high, as_far, ar_far,
    bs_first, br_first, bs_second, br_second, bs_far, br_far, bs_plane, br_plane,
    ps_up, ps_down, pr_up, pr_down, qs_up, qs_down, qr_up, qr_down,
    zs_in, zr_in, zs_pair, zr_pair, zs_out, zr_out,
):
    layer, row, col = lax.axis_index("layer"), lax.axis_index("row"), lax.axis_index("col")
    zh, core = lax.div(row, 2), lax.rem(row, 2)
    y, x = lax.div(col, 4), lax.rem(col, 4)
    ga = x + core * (y - x)
    gb = y + core * (x - y)

    def at(a, b):
        return {"col": (1 - core) * (b * 4 + a) + core * (a * 4 + b)}

    a_up, a_down = at(lax.rem(ga + 1, 4), gb), at(lax.rem(ga + 3, 4), gb)
    b_up, b_down = at(ga, lax.rem(gb + 1, 4)), at(ga, lax.rem(gb + 3, 4))
    step = 1 - 2 * core
    zh_first, zh_second = lax.rem(zh + step + 4, 4), lax.rem(zh - step + 4, 4)
    z_first, z_second = {"row": zh_first * 2 + core}, {"row": zh_second * 2 + core}
    outer = jnp.logical_or(layer == 0, layer == 3)
    inner = jnp.logical_not(outer)
    z_inner = {"layer": 1 + lax.div(layer, 2)}
    z_partner = {"layer": lax.rem(3 - layer, 4)}
    z_outer = {"layer": lax.rem(3 * layer + 1, 4)}

    load_e = pltpu.make_async_copy(e_hbm, e_ref, in_sems.at[0])
    load_a = pltpu.make_async_copy(a_hbm, a_ref, in_sems.at[1])
    load_e.start()
    load_a.start()

    barrier = pltpu.get_barrier_semaphore()

    def greet(device):
        pl.semaphore_signal(barrier, inc=1, device_id=device, device_id_type=MESH)

    for device in (z_first, z_second, a_up, a_down, b_up, b_down):
        greet(device)

    @pl.when(outer)
    def _():
        greet(z_inner)

    @pl.when(inner)
    def _():
        greet(z_partner)
        greet(z_outer)

    @pl.when(core == 0)
    def _():
        for yy in range(4):
            greet({"row": zh * 2 + 1, "col": yy * 4 + x})
        for d in range(1, 4):
            greet({"row": zh * 2, "col": lax.rem(y + d, 4) * 4 + x})

    @pl.when(core == 1)
    def _():
        for d in range(1, 4):
            greet({"row": zh * 2 + lax.div(x, 2), "col": y * 4 + lax.rem(x + d, 4)})

        @pl.when(x < 2)
        def _():
            greet({"row": zh * 2})

    load_e.wait()
    for q in range(2):
        left, right = swap(e_ref[q, :HALF, :], e_ref[q, HALF:, :])
        b_mine[0, q] = left
        b_mine[1, q] = right
    with jax.named_scope("barrier"):
        pl.semaphore_wait(barrier, 6 + (2 - outer.astype(jnp.int32)) + 3 + core + 2 - core * lax.div(x, 2))

    firsts = [remote(b_mine.at[h], b_first.at[h], bs_first.at[h], br_first.at[h], z_first) for h in range(2)]
    seconds = [remote(b_mine.at[h], b_second.at[h], bs_second.at[h], br_second.at[h], z_second) for h in range(2)]
    b_fars = [remote(b_first.at[h], b_far.at[h], bs_far.at[h], br_far.at[h], z_first) for h in range(2)]
    rows = [pl.ds(p * (a_ref.shape[0] // PIECES), a_ref.shape[0] // PIECES) for p in range(PIECES)]
    ups = [remote(a_ref.at[r], a_low.at[r], as_up.at[p], ar_low.at[p], a_up) for p, r in enumerate(rows)]
    downs = [remote(a_ref.at[r], a_high.at[r], as_down.at[p], ar_high.at[p], a_down) for p, r in enumerate(rows)]
    a_fars = [
        remote(a_high.at[r], a_far.at[r], as_far.at[p], ar_far.at[p], a_down) if p % 2
        else remote(a_low.at[r], a_far.at[r], as_far.at[p], ar_far.at[p], a_up)
        for p, r in enumerate(rows)
    ]

    def relay(p):
        (downs if p % 2 else ups)[p].wait_recv()
        a_fars[p].start()

    blocks = ((b_mine, zh), (b_first, zh_second), (b_second, zh_first), (b_far, lax.rem(zh + 2, 4)))

    def exchange(h, k, end=False):
        held, source = blocks[k]
        src, base = held.at[h], 12 * h + 3 * k
        copies = [(
            jnp.logical_and(core == 0, source == y), src, b_all.at[h, pl.ds(2 * core, 2), y],
            bs_plane.at[base], br_plane.at[4 * h + y], {"row": zh * 2, "col": source * 4 + x},
        )]
        for q in range(2):
            copies.append((
                jnp.logical_and(core == 1, x == 2 * core + q), src.at[q], b_all.at[h, source, x],
                bs_plane.at[base + 1 + q], br_plane.at[4 * h + x], {"row": zh * 2 + 1, "col": y * 4 + 2 * core + q},
            ))
        for own, src, dst, send, recv, device in copies:
            @pl.when(jnp.logical_not(own))
            def _():
                copy = remote(src, dst, send, recv, device)
                if end:
                    copy.wait_send()
                else:
                    copy.start()

            if not end:
                @pl.when(own)
                def _():
                    pltpu.make_async_copy(src, dst, recv).start()

    firsts[0].start()
    exchange(0, 0)
    load_a.wait()
    for p in range(2):
        ups[p].start()
        downs[p].start()
    with jax.named_scope("b_sent0"):
        firsts[0].wait_send()
    seconds[0].start()
    with jax.named_scope("relay0"):
        relay(0)
    ups[2].start()
    downs[2].start()
    with jax.named_scope("b_first0"):
        firsts[0].wait_recv()
    b_fars[0].start()
    firsts[1].start()
    exchange(0, 1)
    with jax.named_scope("relay1"):
        relay(1)
    with jax.named_scope("b_second0"):
        seconds[0].wait_recv()
    exchange(0, 2)
    ups[3].start()
    downs[3].start()
    with jax.named_scope("b_sent1"):
        firsts[1].wait_send()
    seconds[1].start()
    with jax.named_scope("b_far0"):
        b_fars[0].wait_recv()
    exchange(0, 3)
    with jax.named_scope("relay2"):
        relay(2)
    with jax.named_scope("b_first1"):
        firsts[1].wait_recv()
    b_fars[1].start()
    with jax.named_scope("relay3"):
        relay(3)

    def factor(h):
        for j in range(4):
            n = lax.rem(gb + j, 4)
            drain(b_all.at[h, :, n], br_plane.at[4 * h + n])
        for j in range(0, 4, 2):
            for i in range(4):
                k = lax.rem(ga + i, 4)
                both = swap(b_all[h, k, lax.rem(gb + j, 4)], b_all[h, k, lax.rem(gb + j + 1, 4)])
                for r, block in enumerate(both):
                    hi, lo = parts(block)
                    cols = pl.ds(j * HALF, BK)
                    b_cat[pl.ds(i * BK + r * HALF, HALF), cols] = hi
                    b_cat[pl.ds(512 + i * BK + r * HALF, HALF), cols] = lo
                    b_cat[pl.ds(1024 + i * BK + r * HALF, HALF), cols] = hi

    size = a_ref.shape[0] // ITEMS
    part = size // 2

    def span(m):
        return pl.ds(pl.multiple_of(m * size, size), size)

    def top(m):
        return pl.ds(pl.multiple_of(m * part, part), part)

    def multiply(t):
        m = lax.rem(t, CHUNKS)
        r = pl.ds(pl.multiple_of(m * 2 * size, 2 * size), 2 * size)
        pairs = [parts(ref[r, :]) for ref in (a_ref, a_high, a_far, a_low)]
        his, los = [p[0] for p in pairs], [p[1] for p in pairs]
        left = jnp.concatenate(his + his + los, axis=1)
        out = jnp.dot(left, b_cat[...], preferred_element_type=jnp.float32)
        mine, above = swap(out[:size, :BK], out[size:, :BK])
        far, below = swap(out[:size, BK:], out[size:, BK:])
        keep[span(t), :] = mine
        late_up[top(t), :] = above[:part]
        late_down[top(t), :] = below[part:]
        go_up[t, 0], go_up[t, 1] = far[:part], above[part:]
        go_down[t, 0], go_down[t, 1] = far[part:], below[:part]
        remote(go_up.at[t], in_up.at[t], ps_up, pr_up.at[t], b_up).start()
        remote(go_down.at[t], in_down.at[t], ps_down, pr_down.at[t], b_down).start()

    def pass_on(m):
        drain(in_up.at[m], pr_up.at[m])
        late_up[top(m), :] += in_up[m, 0]
        remote(late_up.at[top(m)], end_up.at[top(m)], qs_up, qr_up.at[m], b_up).start()
        drain(in_down.at[m], pr_down.at[m])
        late_down[top(m), :] += in_down[m, 0]
        remote(late_down.at[top(m)], end_down.at[top(m)], qs_down, qr_down.at[m], b_down).start()

    def close_layer(m):
        drain(end_up.at[top(m)], qr_up.at[m])
        drain(end_down.at[top(m)], qr_down.at[m])
        low, high = top(2 * m), top(2 * m + 1)
        z_mine[low, :] = keep[low, :] + (end_up[top(m), :] + in_down[m, 1])
        z_mine[high, :] = keep[high, :] + (in_up[m, 1] + end_down[top(m), :])

        @pl.when(outer)
        def _():
            remote(z_mine.at[span(m)], z_in.at[span(m)], zs_in, zr_in.at[m], z_inner).start()

    def pair_up(m):
        drain(z_in.at[span(m)], zr_in.at[m])
        z_pair[span(m), :] = z_mine[span(m), :] + z_in[span(m), :]
        remote(z_pair.at[span(m)], z_other.at[span(m)], zs_pair, zr_pair.at[m], z_partner).start()

    def unpack(m):
        first, second = swap(z_sum[span(m - CHUNKS), :], z_sum[span(m), :])
        o_ref[span(2 * (m - CHUNKS)), :] = first
        o_ref[span(2 * (m - CHUNKS) + 1), :] = second
        r = pl.ds(pl.multiple_of(2 * (m - CHUNKS) * size, size), 2 * size)
        pltpu.make_async_copy(o_ref.at[r], o_hbm.at[r], out_sem).start()

    def finish(m):
        drain(z_other.at[span(m)], zr_pair.at[m])
        z_sum[span(m), :] = z_pair[span(m), :] + z_other[span(m), :]
        remote(z_sum.at[span(m)], z_sum.at[span(m)], zs_out, zr_out.at[m], z_outer).start()
        pl.when(m >= CHUNKS)(lambda: unpack(m))

    with jax.named_scope("factor0"):
        factor(0)

    stages = ((multiply, 0, None), (pass_on, 2, None), (close_layer, 4, None), (pair_up, 7, inner), (finish, 10, inner))

    def body(t, carry):
        @pl.when(jnp.logical_and(lax.rem(t, CHUNKS // PIECES) == 0, t < CHUNKS))
        def _():
            p = lax.div(t, CHUNKS // PIECES)
            r = pl.ds(pl.multiple_of(p * (a_ref.shape[0] // PIECES), 8), a_ref.shape[0] // PIECES)
            drain(a_far.at[r], ar_far.at[p])

            @pl.when(lax.rem(p, 2) == 0)
            def _():
                drain(a_high.at[r], ar_high.at[p])

            @pl.when(lax.rem(p, 2) == 1)
            def _():
                drain(a_low.at[r], ar_low.at[p])

        @pl.when(t == 2)
        def _():
            exchange(1, 0)
            exchange(1, 1)
            with jax.named_scope("b_second1"):
                seconds[1].wait_recv()
            exchange(1, 2)

        @pl.when(t == 4)
        def _():
            with jax.named_scope("b_far1"):
                b_fars[1].wait_recv()
            exchange(1, 3)

        @pl.when(t == CHUNKS)
        def _():
            with jax.named_scope("factor1"):
                factor(1)

        for stage, lag, cond in stages:
            m = t - lag
            ok = jnp.logical_and(m >= 0, m < ITEMS)
            if cond is not None:
                ok = jnp.logical_and(ok, cond)
            pl.when(ok)(lambda stage=stage, m=m: jax.named_scope(stage.__name__)(stage)(m))
        return carry

    lax.fori_loop(0, ITEMS + stages[-1][1], body, 0)

    with jax.named_scope("outs"):
        @pl.when(outer)
        def _():
            def take(m, carry):
                drain(z_sum.at[span(m)], zr_out.at[m])
                pl.when(m >= CHUNKS)(lambda: unpack(m))
                return carry

            lax.fori_loop(0, ITEMS, take, 0)
            drain(z_mine, zs_in)

        @pl.when(inner)
        def _():
            drain(z_pair, zs_pair)
            drain(z_sum, zs_out)

    with jax.named_scope("sends"):
        pltpu.make_async_copy(o_ref, o_hbm, out_sem).wait()
        for ref, sem in ((go_up, ps_up), (go_down, ps_down), (late_up, qs_up), (late_down, qs_down)):
            drain(ref, sem)
        for c in seconds + b_fars + ups + downs + a_fars:
            c.wait_send()
        for h in range(2):
            for k in range(4):
                exchange(h, k, end=True)


def local(panels, eigvecs):
    m, f32 = panels.shape[0], jnp.float32
    whole = pltpu.VMEM((m, BK), f32)
    block = pltpu.VMEM((2, 2, HALF, BK), f32)
    dma = pltpu.SemaphoreType.DMA
    both = pltpu.VMEM((ITEMS, 2, m // ITEMS // 2, BK), f32)
    late = pltpu.VMEM((m // 2, BK), f32)
    pieces, items = dma((PIECES,)), dma((ITEMS,))
    return pl.pallas_call(
        kernel,
        out_shape=jax.ShapeDtypeStruct((m, BK), f32),
        in_specs=[pl.BlockSpec(memory_space=pltpu.HBM)] * 2,
        out_specs=pl.BlockSpec(memory_space=pl.ANY),
        scratch_shapes=[
            whole, pltpu.VMEM((2, BK, BK), f32), whole, whole, whole, block, block, block, block,
            pltpu.VMEM((2, 4, 4, HALF, BK), f32), pltpu.VMEM((12 * BK, 2 * BK), jnp.bfloat16), whole,
            both, both, both, both, late, late, late, late, whole, whole, whole, whole, whole, whole,
            dma((2,)), dma, pieces, pieces, pieces, pieces, pieces, pieces,
            dma((2,)), dma((2,)), dma((2,)), dma((2,)), dma((2,)), dma((2,)), dma((24,)), dma((8,)),
            dma, dma, items, items, dma, dma, items, items,
            dma, items, dma, items, dma, items,
        ],
        compiler_params=pltpu.CompilerParams(collective_id=0, has_side_effects=True, vmem_limit_bytes=53 * 2**20),
        name="panels_by_vectors",
    )(panels, eigvecs.reshape(2, BK, BK))


def solution(mesh):
    in_specs = (P("row", ("layer", "col")), P(("layer", "row"), "col"))
    return jax.shard_map(local, mesh=mesh, in_specs=in_specs, out_specs=P("row", "col"), check_vma=False)
```

```python
import jax
import jax.numpy as jnp
from jax import lax
from jax.experimental import pallas as pl
from jax.experimental.pallas import tpu as pltpu
from jax.sharding import PartitionSpec as P

MESH = pl.DeviceIdType.MESH
BK = 128
QUARTERS = 4
QUARTER = BK // QUARTERS
PIECES = 4
ITEMS = QUARTERS * PIECES
LAGS = (2, 5, 8, 11)


def remote(src, dst, send, recv, device):
    return pltpu.make_async_remote_copy(src_ref=src, dst_ref=dst, send_sem=send, recv_sem=recv, device_id=device, device_id_type=MESH)


def drain(ref, sem):
    pltpu.make_async_copy(ref, ref, sem).wait()


def parts(x):
    hi = x.astype(jnp.bfloat16)
    return hi, (x - hi.astype(jnp.float32)).astype(jnp.bfloat16)


def swap(a, b, width):
    even = lax.rem(lax.div(lax.broadcasted_iota(jnp.int32, a.shape, 1), width), 2) == 0
    return jnp.where(even, a, pltpu.roll(b, width, 1)), jnp.where(even, pltpu.roll(a, BK - width, 1), b)


def turn(x):
    a, b = swap(x[0], x[2], 2 * QUARTER)
    c, d = swap(x[1], x[3], 2 * QUARTER)
    return (*swap(a, c, QUARTER), *swap(b, d, QUARTER))


def kernel(
    a_hbm, e_hbm, o_hbm,
    a_ref, e_ref, o_ref, a_low, a_high, a_far, a_cat, b_mine, b_first, b_second, b_far, b_all, b_cat, keep,
    go_up, go_down, in_up, in_down, late_up, late_down, end_up, end_down, z_mine, z_in, z_pair, z_other, z_sum,
    in_sems, out_sem, plane_sem, z_sem, as_near, as_far, ar_low, ar_high, ar_far,
    bs_lead, bs_first, bs_second, bs_far, br_first, br_second, br_far, bs_plane, br_plane,
    ps_up, ps_down, pr, qs_up, qs_down, qr, zs_in, zr_in, zs_pair, zr_pair, zs_out, zr_out,
):
    layer, row, col = lax.axis_index("layer"), lax.axis_index("row"), lax.axis_index("col")
    zh, core = lax.div(row, 2), lax.rem(row, 2)
    y, x = lax.div(col, 4), lax.rem(col, 4)
    ga = x + core * (y - x)
    gb = y + core * (x - y)

    def at(a, b):
        return {"col": (1 - core) * (b * 4 + a) + core * (a * 4 + b)}

    a_up, a_down = at(lax.rem(ga + 1, 4), gb), at(lax.rem(ga + 3, 4), gb)
    b_up, b_down = at(ga, lax.rem(gb + 1, 4)), at(ga, lax.rem(gb + 3, 4))
    step = 1 - 2 * core
    zh_first, zh_second = lax.rem(zh + step + 4, 4), lax.rem(zh - step + 4, 4)
    z_first, z_second = {"row": zh_first * 2 + core}, {"row": zh_second * 2 + core}
    outer = jnp.logical_or(layer == 0, layer == 3)
    inner = jnp.logical_not(outer)
    z_inner = 1 + lax.div(layer, 2)
    z_partner = lax.rem(3 - layer, 4)
    z_outer = lax.rem(3 * layer + 1, 4)
    early = zh < 2
    lead = early.astype(jnp.int32)

    load_e = pltpu.make_async_copy(e_hbm, e_ref, in_sems.at[0])
    load_a = pltpu.make_async_copy(a_hbm, a_ref, in_sems.at[1])
    load_e.start()
    load_a.start()

    barrier = pltpu.get_barrier_semaphore()

    def greet(device):
        pl.semaphore_signal(barrier, inc=1, device_id=device, device_id_type=MESH)

    core0, core1 = zh * 2, zh * 2 + 1
    for d in (1, 3):
        greet({"row": lax.rem(zh + d, 4) * 2})

    @pl.when(outer)
    def _():
        greet({"row": core0, "layer": z_inner})

    @pl.when(inner)
    def _():
        greet({"row": core0, "layer": z_partner})
        greet({"row": core0, "layer": z_outer})

    for d in (1, 3, 2):
        greet({"row": core1, "col": y * 4 + lax.rem(x + d, 4)})
        greet({"row": core1, "col": lax.rem(y + d, 4) * 4 + x})

    @pl.when(core == 0)
    def _():
        greet({"row": core1})

    @pl.when(core == 1)
    def _():
        greet({"row": core0})

    load_e.wait()
    for h in range(2):
        for q, packed in enumerate(turn([e_ref[h, pl.ds(g * QUARTER, QUARTER), :] for g in range(4)])):
            b_mine[q, h] = packed

    with jax.named_scope("plane_barrier"):
        @pl.when(core == 1)
        def _():
            pl.semaphore_wait(barrier, 13)
            pl.semaphore_signal(plane_sem, inc=1, device_id={"row": core0}, device_id_type=MESH)

        @pl.when(core == 0)
        def _():
            pl.semaphore_wait(plane_sem, 1)

    rows = [pl.ds(p * (a_ref.shape[0] // PIECES), a_ref.shape[0] // PIECES) for p in range(PIECES)]
    ups = [remote(a_ref.at[r], a_low.at[r], as_near, ar_low.at[p], a_up) for p, r in enumerate(rows)]
    downs = [remote(a_ref.at[r], a_high.at[r], as_near, ar_high.at[p], a_down) for p, r in enumerate(rows)]
    a_fars = [
        remote(a_high.at[r], a_far.at[r], as_far, ar_far.at[p], a_down) if p % 2
        else remote(a_low.at[r], a_far.at[r], as_far, ar_far.at[p], a_up)
        for p, r in enumerate(rows)
    ]

    def send_piece(p):
        ups[p].start()
        downs[p].start()

    def relay(p):
        with jax.named_scope(f"relay{p}"):
            (downs if p % 2 else ups)[p].wait_recv()
        a_fars[p].start()

    firsts = [remote(b_mine.at[q], b_first.at[q], bs_first if q else bs_lead, br_first.at[q], z_first) for q in range(QUARTERS)]
    seconds = [remote(b_mine.at[q], b_second.at[q], bs_second, br_second.at[q], z_second) for q in range(QUARTERS)]
    b_fars = [remote(b_first.at[q], b_far.at[q], bs_far, br_far.at[q], z_first) for q in range(QUARTERS)]
    blocks = ((b_mine, zh), (b_first, zh_second), (b_second, zh_first), (b_far, lax.rem(zh + 2, 4)))

    def exchange(q, k):
        held, source = blocks[k]
        src = held.at[q]
        copies = [(jnp.logical_and(core == 0, source == y), src, b_all.at[q, pl.ds(2 * core, 2), y], {"row": core0, "col": source * 4 + x})]
        for h in range(2):
            copies.append((
                jnp.logical_and(core == 1, x == 2 * core + h), src.at[h], b_all.at[q, source, x], {"row": core1, "col": y * 4 + 2 * core + h},
            ))
        for own, src, dst, device in copies:
            @pl.when(own)
            def _():
                pltpu.make_async_copy(src, dst, br_plane.at[q]).start()

            @pl.when(jnp.logical_not(own))
            def _():
                remote(src, dst, bs_plane, br_plane.at[q], device).start()

    def arrived(copies, q):
        name = "b_first" if copies is firsts else "b_second" if copies is seconds else "b_far"
        with jax.named_scope(f"{name}{q}"):
            copies[q].wait_recv()

    exchange(0, 0)
    load_a.wait()
    send_piece(0)
    send_piece(1)

    @pl.when(early)
    def _():
        send_piece(2)
        send_piece(3)

    @pl.when(zh == 0)
    def _():
        relay(0)

    with jax.named_scope("z_barrier"):
        @pl.when(core == 0)
        def _():
            pl.semaphore_wait(barrier, 7 + 2 * inner.astype(jnp.int32))
            pl.semaphore_signal(z_sem, inc=1, device_id={"row": core1}, device_id_type=MESH)

        @pl.when(core == 1)
        def _():
            pl.semaphore_wait(z_sem, 1)

    firsts[0].start()
    with jax.named_scope("b_lead"):
        firsts[0].wait_send()
    seconds[0].start()
    firsts[1].start()
    arrived(firsts, 0)
    b_fars[0].start()
    firsts[2].start()
    exchange(0, 1)
    pl.when(zh != 0)(lambda: relay(0))
    pl.when(zh == 0)(lambda: relay(1))
    arrived(seconds, 0)
    exchange(0, 2)
    seconds[1].start()
    arrived(firsts, 1)
    b_fars[1].start()
    pl.when(zh != 0)(lambda: relay(1))
    pl.when(early)(lambda: relay(2))
    pl.when(jnp.logical_not(early))(lambda: send_piece(2))
    arrived(b_fars, 0)
    exchange(0, 3)
    firsts[3].start()
    exchange(1, 0)
    exchange(1, 1)
    arrived(firsts, 2)
    b_fars[2].start()
    seconds[2].start()
    pl.when(early)(lambda: relay(3))

    @pl.when(jnp.logical_not(early))
    def _():
        relay(2)
        send_piece(3)

    arrived(seconds, 1)
    exchange(1, 2)

    def factor(q):
        with jax.named_scope(f"factor{q}"):
            drain(b_all.at[q], br_plane.at[q])
            for i in range(4):
                k = lax.rem(ga + i, 4)
                for g, block in enumerate(turn([b_all[q, k, lax.rem(gb + j, 4)] for j in range(4)])):
                    hi, lo = parts(block)
                    for r in (i * BK + g * QUARTER, 4 * BK + i * BK + g * QUARTER):
                        b_cat[q, pl.ds(r, QUARTER), pl.ds(0, BK)] = hi
                        b_cat[q, pl.ds(r, QUARTER), pl.ds(BK, BK)] = lo

    size = a_ref.shape[0] // ITEMS
    part = size // 2

    def span(m):
        return pl.ds(pl.multiple_of(m * size, size), size)

    def top(m):
        return pl.ds(pl.multiple_of(m * part, part), part)

    def place(t):
        b, c = lax.div(t, 9), lax.div(t, 12)
        q = (1 - b) * lax.div(t, 3) + (b - c) * (t - 9) + c * 3
        p = (1 - b) * lax.rem(t, 3) + (b - c) * 3 + c * (t - 12)
        return lead * lax.div(t, PIECES) + (1 - lead) * q, lead * lax.rem(t, PIECES) + (1 - lead) * p

    def item(q, p):
        b = lax.div(p, 3)
        return lead * (PIECES * q + p) + (1 - lead) * ((1 - b) * (3 * q + p) + b * (9 + q))

    def whole(p):
        return pl.ds(pl.multiple_of(p * 4 * size, 4 * size), 4 * size)

    def take_piece(p):
        r = whole(p)
        with jax.named_scope("piece"):
            drain(a_far.at[r], ar_far.at[p])

            @pl.when(lax.rem(p, 2) == 0)
            def _():
                drain(a_high.at[r], ar_high.at[p])

            @pl.when(lax.rem(p, 2) == 1)
            def _():
                drain(a_low.at[r], ar_low.at[p])

        for i, ref in enumerate((a_ref, a_high, a_far, a_low)):
            hi, lo = parts(ref[r, :])
            a_cat[r, pl.ds(i * BK, BK)] = hi
            a_cat[r, pl.ds((4 + i) * BK, BK)] = lo

    def multiply(t):
        q, p = place(t)
        pl.when(q == 0)(lambda: take_piece(p))
        out = jnp.dot(a_cat[whole(p), :], b_cat[q], preferred_element_type=jnp.float32)
        out = out[:, :BK] + out[:, BK:]
        mine, above, far, below = turn([out[g * size:(g + 1) * size] for g in range(4)])
        keep[span(t), :] = mine
        late_up[top(t), :] = above[:part]
        late_down[top(t), :] = below[part:]
        go_up[t, 0], go_up[t, 1] = far[:part], above[part:]
        go_down[t, 0], go_down[t, 1] = far[part:], below[:part]
        remote(go_up.at[t], in_up.at[t], ps_up, pr.at[t, 0], b_up).start()
        remote(go_down.at[t], in_down.at[t], ps_down, pr.at[t, 1], b_down).start()

    def pass_on(m):
        drain(in_up.at[m], pr.at[m, 0])
        late_up[top(m), :] += in_up[m, 0]
        remote(late_up.at[top(m)], end_up.at[top(m)], qs_up, qr.at[m], b_up).start()
        drain(in_down.at[m], pr.at[m, 1])
        late_down[top(m), :] += in_down[m, 0]
        remote(late_down.at[top(m)], end_down.at[top(m)], qs_down, qr.at[m], b_down).start()

    def close_layer(m):
        drain(z_mine.at[span(m)], qr.at[m])
        low, high = top(2 * m), top(2 * m + 1)
        z_mine[low, :] = keep[low, :] + (end_up[top(m), :] + in_down[m, 1])
        z_mine[high, :] = keep[high, :] + (in_up[m, 1] + end_down[top(m), :])

        @pl.when(outer)
        def _():
            remote(z_mine.at[span(m)], z_in.at[span(m)], zs_in, zr_in.at[m], {"layer": z_inner}).start()

    def pair_up(m):
        drain(z_in.at[span(m)], zr_in.at[m])
        z_pair[span(m), :] = z_mine[span(m), :] + z_in[span(m), :]
        remote(z_pair.at[span(m)], z_other.at[span(m)], zs_pair, zr_pair.at[m], {"layer": z_partner}).start()

    def unpack(t):
        q, p = place(t)

        @pl.when(q == 3)
        def _():
            for g, block in enumerate(turn([z_sum[span(m), :] for m in [item(i, p) for i in range(QUARTERS - 1)] + [t]])):
                o_ref[span(4 * p + g), :] = block
            pltpu.make_async_copy(o_ref.at[whole(p)], o_hbm.at[whole(p)], out_sem).start()

    def finish(m):
        drain(z_other.at[span(m)], zr_pair.at[m])
        z_sum[span(m), :] = z_pair[span(m), :] + z_other[span(m), :]
        remote(z_sum.at[span(m)], z_sum.at[span(m)], zs_out, zr_out.at[m], {"layer": z_outer}).start()
        unpack(m)

    def run(stage, m):
        jax.named_scope(stage.__name__)(stage)(m)

    factor(0)
    run(multiply, 0)
    arrived(b_fars, 1)
    exchange(1, 3)
    run(multiply, 1)
    exchange(2, 0)
    exchange(2, 1)
    arrived(seconds, 2)
    exchange(2, 2)
    arrived(firsts, 3)
    b_fars[3].start()
    seconds[3].start()
    pl.when(jnp.logical_not(early))(lambda: run(pass_on, 0))
    run(multiply, 2)
    pl.when(early)(lambda: run(pass_on, 0))
    pl.when(jnp.logical_not(early))(lambda: relay(3))
    arrived(b_fars, 2)
    exchange(2, 3)
    pl.when(jnp.logical_not(early))(lambda: factor(1))
    run(multiply, 3)
    run(pass_on, 1)
    stages = tuple(zip((multiply, pass_on, close_layer, pair_up, finish), (0, *LAGS), (4, 2, 0, 0, 0), (None, None, None, inner, inner)))

    def body(t, carry):
        pl.when(jnp.logical_and(early, t == 4))(lambda: factor(1))
        pl.when(t == 6 + 2 * lead)(lambda: factor(2))

        @pl.when(t == 5)
        def _():
            exchange(3, 0)
            exchange(3, 1)

        @pl.when(t == 6)
        def _():
            arrived(seconds, 3)
            exchange(3, 2)

        @pl.when(t == 7)
        def _():
            arrived(b_fars, 3)
            exchange(3, 3)

        pl.when(t == 12)(lambda: factor(3))
        for stage, lag, least, cond in stages:
            m = t - lag
            ok = jnp.logical_and(m >= least, m < ITEMS)
            if cond is not None:
                ok = jnp.logical_and(ok, cond)
            pl.when(ok)(lambda stage=stage, m=m: run(stage, m))
        return carry

    lax.fori_loop(4, ITEMS + LAGS[-1], body, 0)

    with jax.named_scope("outs"):
        @pl.when(outer)
        def _():
            def take(m, carry):
                drain(z_sum.at[span(m)], zr_out.at[m])
                unpack(m)
                return carry

            lax.fori_loop(0, ITEMS, take, 0)
            drain(z_mine, zs_in)

        @pl.when(inner)
        def _():
            drain(z_pair, zs_pair)
            drain(z_sum, zs_out)

    with jax.named_scope("sends"):
        for ref, sem in ((go_up, ps_up), (go_down, ps_down), (late_up, qs_up), (late_down, qs_down)):
            drain(ref, sem)
        drain(a_ref, as_near)
        drain(a_ref, as_near)
        drain(a_far, as_far)
        drain(b_mine.at[pl.ds(1, 3)], bs_first)
        drain(b_mine, bs_second)
        drain(b_first, bs_far)
        for own, sent in ((core == 0, 14), (jnp.logical_and(core == 1, x < 2), 16), (jnp.logical_and(core == 1, x >= 2), 12)):
            pl.when(own)(lambda sent=sent: drain(a_ref.at[pl.ds(0, sent * BK)], bs_plane))
        pltpu.make_async_copy(o_ref, o_hbm, out_sem).wait()


def local(panels, eigvecs):
    m, f32, bf16 = panels.shape[0], jnp.float32, jnp.bfloat16
    whole = pltpu.VMEM((m, BK), f32)
    block = pltpu.VMEM((QUARTERS, 2, QUARTER, BK), f32)
    both = pltpu.VMEM((ITEMS, 2, m // ITEMS // 2, BK), f32)
    late = pltpu.VMEM((m // 2, BK), f32)
    dma, regular = pltpu.SemaphoreType.DMA, pltpu.SemaphoreType.REGULAR
    four, items = dma((4,)), dma((ITEMS,))
    return pl.pallas_call(
        kernel,
        out_shape=jax.ShapeDtypeStruct((m, BK), f32),
        in_specs=[pl.BlockSpec(memory_space=pltpu.HBM)] * 2,
        out_specs=pl.BlockSpec(memory_space=pl.ANY),
        scratch_shapes=[
            whole, pltpu.VMEM((2, BK, BK), f32), whole, whole, whole, whole, pltpu.VMEM((m, 8 * BK), bf16), block, block, block, block,
            pltpu.VMEM((QUARTERS, 4, 4, QUARTER, BK), f32), pltpu.VMEM((QUARTERS, 8 * BK, 2 * BK), bf16), whole,
            both, both, both, both, late, late, late, late, whole, whole, whole, whole, whole,
            dma((2,)), dma, regular, regular, dma, dma, four, four, four,
            dma, dma, dma, dma, four, four, four, dma, four,
            dma, dma, dma((ITEMS, 2)), dma, dma, items, dma, items, dma, items, dma, items,
        ],
        compiler_params=pltpu.CompilerParams(collective_id=0, has_side_effects=True, vmem_limit_bytes=52 * 2**20),
        name="panels_by_vectors",
    )(panels, eigvecs.reshape(2, BK, BK))


def solution(mesh):
    in_specs = (P("row", ("layer", "col")), P(("layer", "row"), "col"))
    return jax.shard_map(local, mesh=mesh, in_specs=in_specs, out_specs=P("row", "col"), check_vma=False)
```

```python
import jax
import jax.numpy as jnp
from jax import lax
from jax.experimental import pallas as pl
from jax.experimental.pallas import tpu as pltpu
from jax.sharding import PartitionSpec as P

MESH = pl.DeviceIdType.MESH
BK = 128
QUARTERS = 4
QUARTER = BK // QUARTERS
PIECES = 4
ITEMS = QUARTERS * PIECES
SPLIT = 4
LAGS = (3, 6, 8, 11)
SLOWER = {"pass_on": (8,), "close_layer": (8, 10)}


def remote(src, dst, send, recv, device):
    return pltpu.make_async_remote_copy(src_ref=src, dst_ref=dst, send_sem=send, recv_sem=recv, device_id=device, device_id_type=MESH)


def drain(ref, sem):
    pltpu.make_async_copy(ref, ref, sem).wait()


def parts(x):
    hi = x.astype(jnp.bfloat16)
    return hi, (x - hi.astype(jnp.float32)).astype(jnp.bfloat16)


def swap(a, b, width):
    even = lax.rem(lax.div(lax.broadcasted_iota(jnp.int32, a.shape, 1), width), 2) == 0
    return jnp.where(even, a, pltpu.roll(b, width, 1)), jnp.where(even, pltpu.roll(a, BK - width, 1), b)


def turn(x):
    a, b = swap(x[0], x[2], 2 * QUARTER)
    c, d = swap(x[1], x[3], 2 * QUARTER)
    return (*swap(a, c, QUARTER), *swap(b, d, QUARTER))


def kernel(
    a_hbm, e_hbm, o_hbm,
    a_ref, e_ref, o_ref, a_low, a_high, a_far, a_cat, b_mine, b_first, b_second, b_far, b_all, b_cat, keep,
    go_up, go_down, in_up, in_down, late_up, late_down, end_up, end_down, z_mine, z_in, z_pair, z_other, z_sum,
    in_sems, out_sem, plane_sem, z_sem, as_near, as_far, ar_low, ar_high, ar_far,
    bs_lead, bs_first, bs_second, bs_far, br_first, br_second, br_far, bs_plane, br_plane,
    ps_up, ps_down, pr, qs_up, qs_down, qr, zs_in, zr_in, zs_pair, zr_pair, zs_out, zr_out,
):
    layer, row, col = lax.axis_index("layer"), lax.axis_index("row"), lax.axis_index("col")
    zh, core = lax.div(row, 2), lax.rem(row, 2)
    y, x = lax.div(col, 4), lax.rem(col, 4)
    ga = x + core * (y - x)
    gb = y + core * (x - y)

    def at(a, b):
        return {"col": (1 - core) * (b * 4 + a) + core * (a * 4 + b)}

    a_up, a_down = at(lax.rem(ga + 1, 4), gb), at(lax.rem(ga + 3, 4), gb)
    b_up, b_down = at(ga, lax.rem(gb + 1, 4)), at(ga, lax.rem(gb + 3, 4))
    step = 1 - 2 * core
    zh_first, zh_second = lax.rem(zh + step + 4, 4), lax.rem(zh - step + 4, 4)
    z_first, z_second = {"row": zh_first * 2 + core}, {"row": zh_second * 2 + core}
    outer = jnp.logical_or(layer == 0, layer == 3)
    inner = jnp.logical_not(outer)
    z_inner = 1 + lax.div(layer, 2)
    z_partner = lax.rem(3 - layer, 4)
    z_outer = lax.rem(3 * layer + 1, 4)
    early = zh < 2
    lead = early.astype(jnp.int32)

    load_e = pltpu.make_async_copy(e_hbm, e_ref, in_sems.at[0])
    load_a = pltpu.make_async_copy(a_hbm, a_ref, in_sems.at[1])
    load_e.start()
    load_a.start()

    barrier = pltpu.get_barrier_semaphore()

    def greet(device):
        pl.semaphore_signal(barrier, inc=1, device_id=device, device_id_type=MESH)

    core0, core1 = zh * 2, zh * 2 + 1
    def greet_z(there, layers):
        greet({"row": there * 2, **layers})
        pl.when(there >= 2)(lambda: greet({"row": there * 2 + 1, **layers}))

    for d in (1, 3):
        greet_z(lax.rem(zh + d, 4), {})

    @pl.when(outer)
    def _():
        greet_z(zh, {"layer": z_inner})

    @pl.when(inner)
    def _():
        greet_z(zh, {"layer": z_partner})
        greet_z(zh, {"layer": z_outer})

    for d in (1, 3, 2):
        greet({"row": core1, "col": y * 4 + lax.rem(x + d, 4)})
        greet({"row": core1, "col": lax.rem(y + d, 4) * 4 + x})

    @pl.when(core == 0)
    def _():
        greet({"row": core1})

    @pl.when(core == 1)
    def _():
        greet({"row": core0})

    load_e.wait()
    for h in range(2):
        for q, packed in enumerate(turn([e_ref[h, pl.ds(g * QUARTER, QUARTER), :] for g in range(4)])):
            b_mine[q, h] = packed

    with jax.named_scope("plane_barrier"):
        @pl.when(core == 1)
        def _():
            pl.semaphore_wait(barrier, 13 + (1 - lead) * (6 + 2 * inner.astype(jnp.int32)))
            pl.semaphore_signal(plane_sem, inc=1, device_id={"row": core0}, device_id_type=MESH)

        @pl.when(core == 0)
        def _():
            pl.semaphore_wait(plane_sem, 1)

    rows = [pl.ds(p * (a_ref.shape[0] // PIECES), a_ref.shape[0] // PIECES) for p in range(PIECES)]
    ups = [remote(a_ref.at[r], a_low.at[r], as_near, ar_low.at[p], a_up) for p, r in enumerate(rows)]
    downs = [remote(a_ref.at[r], a_high.at[r], as_near, ar_high.at[p], a_down) for p, r in enumerate(rows)]
    a_fars = [
        remote(a_high.at[r], a_far.at[r], as_far, ar_far.at[p], a_down) if p % 2
        else remote(a_low.at[r], a_far.at[r], as_far, ar_far.at[p], a_up)
        for p, r in enumerate(rows)
    ]

    def send_piece(p):
        ups[p].start()
        downs[p].start()

    def relay(p):
        with jax.named_scope(f"relay{p}"):
            (downs if p % 2 else ups)[p].wait_recv()
        a_fars[p].start()

    firsts = [remote(b_mine.at[q], b_first.at[q], bs_first if q else bs_lead, br_first.at[q], z_first) for q in range(QUARTERS)]
    seconds = [remote(b_mine.at[q], b_second.at[q], bs_second, br_second.at[q], z_second) for q in range(QUARTERS)]
    b_fars = [remote(b_first.at[q], b_far.at[q], bs_far, br_far.at[q], z_first) for q in range(QUARTERS)]
    blocks = ((b_mine, zh), (b_first, zh_second), (b_second, zh_first), (b_far, lax.rem(zh + 2, 4)))

    def exchange(q, k):
        held, source = blocks[k]
        src = held.at[q]
        copies = [(jnp.logical_and(core == 0, source == y), src, b_all.at[q, pl.ds(2 * core, 2), y], {"row": core0, "col": source * 4 + x})]
        for h in range(2):
            copies.append((
                jnp.logical_and(core == 1, x == 2 * core + h), src.at[h], b_all.at[q, source, x], {"row": core1, "col": y * 4 + 2 * core + h},
            ))
        for own, src, dst, device in copies:
            @pl.when(own)
            def _():
                pltpu.make_async_copy(src, dst, br_plane.at[q]).start()

            @pl.when(jnp.logical_not(own))
            def _():
                remote(src, dst, bs_plane, br_plane.at[q], device).start()

    def arrived(copies, q):
        name = "b_first" if copies is firsts else "b_second" if copies is seconds else "b_far"
        with jax.named_scope(f"{name}{q}"):
            copies[q].wait_recv()

    size = a_ref.shape[0] // ITEMS
    part = size // 2

    def span(m):
        return pl.ds(pl.multiple_of(m * size, size), size)

    def top(m):
        return pl.ds(pl.multiple_of(m * part, part), part)

    def whole(p):
        return pl.ds(pl.multiple_of(p * 4 * size, 4 * size), 4 * size)

    def take_piece(p):
        r = whole(p)
        with jax.named_scope("piece"):
            drain(a_far.at[r], ar_far.at[p])

            @pl.when(lax.rem(p, 2) == 0)
            def _():
                drain(a_high.at[r], ar_high.at[p])

            @pl.when(lax.rem(p, 2) == 1)
            def _():
                drain(a_low.at[r], ar_low.at[p])

        for i, ref in enumerate((a_ref, a_high, a_far, a_low)):
            hi, lo = parts(ref[r, :])
            a_cat[r, pl.ds(i * BK, BK)] = hi
            a_cat[r, pl.ds((4 + i) * BK, BK)] = lo

    exchange(0, 0)
    load_a.wait()
    send_piece(0)
    send_piece(1)

    @pl.when(zh == 0)
    def _():
        send_piece(2)
        send_piece(3)
        relay(0)

    with jax.named_scope("z_barrier"):
        @pl.when(core == 0)
        def _():
            pl.semaphore_wait(barrier, 7 + 2 * inner.astype(jnp.int32))
            pl.when(early)(lambda: pl.semaphore_signal(z_sem, inc=1, device_id={"row": core1}, device_id_type=MESH))

        @pl.when(jnp.logical_and(core == 1, early))
        def _():
            pl.semaphore_wait(z_sem, 1)

    firsts[0].start()
    with jax.named_scope("b_lead"):
        firsts[0].wait_send()
    seconds[0].start()
    firsts[1].start()

    @pl.when(zh == 1)
    def _():
        relay(0)
        send_piece(2)

    arrived(firsts, 0)
    b_fars[0].start()
    firsts[2].start()
    exchange(0, 1)
    pl.when(jnp.logical_not(early))(lambda: relay(0))
    pl.when(early)(lambda: relay(1))
    pl.when(zh == 1)(lambda: send_piece(3))
    arrived(seconds, 0)
    exchange(0, 2)
    seconds[1].start()
    arrived(firsts, 1)
    b_fars[1].start()
    pl.when(early)(lambda: relay(2))

    @pl.when(jnp.logical_not(early))
    def _():
        relay(1)
        send_piece(2)

    arrived(b_fars, 0)
    exchange(0, 3)
    firsts[3].start()
    exchange(1, 0)
    exchange(1, 1)
    take_piece(0)
    arrived(firsts, 2)
    b_fars[2].start()
    seconds[2].start()
    pl.when(early)(lambda: relay(3))

    @pl.when(jnp.logical_not(early))
    def _():
        relay(2)
        send_piece(3)

    arrived(seconds, 1)
    exchange(1, 2)
    take_piece(1)
    arrived(b_fars, 1)
    exchange(1, 3)

    def factor(q):
        with jax.named_scope(f"factor{q}"):
            drain(b_all.at[q], br_plane.at[q])
            for i in range(4):
                k = lax.rem(ga + i, 4)
                for g, block in enumerate(turn([b_all[q, k, lax.rem(gb + j, 4)] for j in range(4)])):
                    hi, lo = parts(block)
                    for r in (i * BK + g * QUARTER, 4 * BK + i * BK + g * QUARTER):
                        b_cat[q, pl.ds(r, QUARTER), pl.ds(0, BK)] = hi
                        b_cat[q, pl.ds(r, QUARTER), pl.ds(BK, BK)] = lo

    def place(t):
        b, c = lax.div(t, 9), lax.div(t, 12)
        q = (1 - b) * lax.div(t, 3) + (b - c) * (t - 9) + c * 3
        p = (1 - b) * lax.rem(t, 3) + (b - c) * 3 + c * (t - 12)
        return lead * lax.div(t, PIECES) + (1 - lead) * q, lead * lax.rem(t, PIECES) + (1 - lead) * p

    def item(q, p):
        b = lax.div(p, 3)
        return lead * (PIECES * q + p) + (1 - lead) * ((1 - b) * (3 * q + p) + b * (9 + q))

    def multiply(t):
        q, p = place(t)
        pl.when(jnp.logical_and(q == 0, p >= 2))(lambda: take_piece(p))
        out = jnp.dot(a_cat[whole(p), :], b_cat[q], preferred_element_type=jnp.float32)
        out = out[:, :BK] + out[:, BK:]
        mine, above, far, below = turn([out[g * size:(g + 1) * size] for g in range(4)])
        keep[span(t), :] = mine
        late_up[top(t), :] = above[:part]
        late_down[top(t), :] = below[part:]
        go_up[t, 0], go_up[t, 1] = far[:part], above[part:]
        go_down[t, 0], go_down[t, 1] = far[part:], below[:part]
        remote(go_up.at[t], in_up.at[t], ps_up, pr.at[t], b_up).start()
        remote(go_down.at[t], in_down.at[t], ps_down, pr.at[t], b_down).start()

    def pass_on(m):
        drain(a_ref.at[pl.ds(0, 2 * size)], pr.at[m])
        late_up[top(m), :] += in_up[m, 0]
        remote(late_up.at[top(m)], end_up.at[top(m)], qs_up, qr.at[m], b_up).start()
        late_down[top(m), :] += in_down[m, 0]
        remote(late_down.at[top(m)], end_down.at[top(m)], qs_down, qr.at[m], b_down).start()

    def close_layer(m):
        drain(z_mine.at[span(m)], qr.at[m])
        low, high = top(2 * m), top(2 * m + 1)
        z_mine[low, :] = keep[low, :] + (end_up[top(m), :] + in_down[m, 1])
        z_mine[high, :] = keep[high, :] + (in_up[m, 1] + end_down[top(m), :])

        def send(r, k):
            pl.when(outer)(lambda: remote(z_mine.at[r], z_in.at[r], zs_in, zr_in.at[k], {"layer": z_inner}).start())

        by_parts(m, send)

    def by_parts(m, act):
        pl.when(m < ITEMS - 1)(lambda: act(span(m), m))

        @pl.when(m == ITEMS - 1)
        def _():
            for i in range(SPLIT):
                act(pl.ds((ITEMS - 1) * size + i * (size // SPLIT), size // SPLIT), ITEMS - 1 + i)

    def pair_up(m):
        def act(r, k):
            drain(z_in.at[r], zr_in.at[k])
            z_pair[r, :] = z_mine[r, :] + z_in[r, :]
            remote(z_pair.at[r], z_other.at[r], zs_pair, zr_pair.at[k], {"layer": z_partner}).start()

        by_parts(m, act)

    def unpack(t):
        q, p = place(t)

        @pl.when(q == 3)
        def _():
            for g, block in enumerate(turn([z_sum[span(m), :] for m in [item(i, p) for i in range(QUARTERS - 1)] + [t]])):
                o_ref[span(4 * p + g), :] = block
            pltpu.make_async_copy(o_ref.at[whole(p)], o_hbm.at[whole(p)], out_sem).start()

    def last(k):
        return (k - ITEMS + PIECES + 1) * lax.div(k, ITEMS - PIECES)

    def finish(m):
        def act(r, k):
            drain(z_other.at[r], zr_pair.at[k])
            z_sum[r, :] = z_pair[r, :] + z_other[r, :]
            remote(z_sum.at[r], z_sum.at[r], zs_out, zr_out.at[last(k)], {"layer": z_outer}).start()

        by_parts(m, act)
        unpack(m)

    def run(stage, m):
        jax.named_scope(stage.__name__)(stage)(m)

    factor(0)
    lax.fori_loop(0, 2, lambda t, carry: (run(multiply, t), carry)[1], 0)

    exchange(2, 0)
    exchange(2, 1)
    arrived(seconds, 2)
    exchange(2, 2)
    arrived(firsts, 3)
    b_fars[3].start()
    seconds[3].start()
    pl.when(jnp.logical_not(early))(lambda: run(pass_on, 0))
    run(multiply, 2)
    pl.when(early)(lambda: run(pass_on, 0))
    pl.when(jnp.logical_not(early))(lambda: relay(3))
    arrived(b_fars, 2)
    exchange(2, 3)
    pl.when(jnp.logical_not(early))(lambda: factor(1))
    run(multiply, 3)
    run(pass_on, 1)
    stages = tuple(zip((multiply, pass_on, close_layer, pair_up, finish), (0, *LAGS), (4, 2, 0, 0, 0), (None, None, None, inner, inner)))

    def body(t, carry):
        pl.when(jnp.logical_and(early, t == 4))(lambda: factor(1))
        pl.when(t == 6 + 2 * lead)(lambda: factor(2))

        @pl.when(t == 5)
        def _():
            exchange(3, 0)
            exchange(3, 1)

        @pl.when(t == 6)
        def _():
            arrived(seconds, 3)
            exchange(3, 2)

        @pl.when(t == 7)
        def _():
            arrived(b_fars, 3)
            exchange(3, 3)

        pl.when(t == 12)(lambda: factor(3))
        for stage, lag, least, cond in stages:
            m = t - lag
            ok = t >= 0
            for turn_at in SLOWER.get(stage.__name__, ()):
                m += (t < turn_at).astype(jnp.int32)
                ok = jnp.logical_and(ok, t != turn_at)
            ok = jnp.logical_and(ok, jnp.logical_and(m >= least, m < ITEMS))
            if cond is not None:
                ok = jnp.logical_and(ok, cond)
            pl.when(ok)(lambda stage=stage, m=m: run(stage, m))
        return carry

    lax.fori_loop(4, ITEMS + LAGS[-1], body, 0)

    with jax.named_scope("outs"):
        @pl.when(outer)
        def _():
            def take(m, carry):
                by_parts(m, lambda r, k: drain(z_sum.at[r], zr_out.at[last(k)]))
                unpack(m)
                return carry

            drain(z_sum.at[pl.ds(0, (ITEMS - PIECES) * size)], zr_out.at[0])
            lax.fori_loop(ITEMS - PIECES, ITEMS, take, 0)
            drain(z_mine, zs_in)

        @pl.when(inner)
        def _():
            drain(z_pair, zs_pair)
            drain(z_sum, zs_out)

    with jax.named_scope("sends"):
        for ref, sem in ((go_up, ps_up), (go_down, ps_down), (late_up, qs_up), (late_down, qs_down)):
            drain(ref, sem)
        drain(a_ref, as_near)
        drain(a_ref, as_near)
        drain(a_far, as_far)
        drain(b_mine.at[pl.ds(1, 3)], bs_first)
        drain(b_mine, bs_second)
        drain(b_first, bs_far)
        for own, sent in ((core == 0, 14), (jnp.logical_and(core == 1, x < 2), 16), (jnp.logical_and(core == 1, x >= 2), 12)):
            pl.when(own)(lambda sent=sent: drain(a_ref.at[pl.ds(0, sent * BK)], bs_plane))
        pltpu.make_async_copy(o_ref, o_hbm, out_sem).wait()


def local(panels, eigvecs):
    m, f32, bf16 = panels.shape[0], jnp.float32, jnp.bfloat16
    whole = pltpu.VMEM((m, BK), f32)
    block = pltpu.VMEM((QUARTERS, 2, QUARTER, BK), f32)
    both = pltpu.VMEM((ITEMS, 2, m // ITEMS // 2, BK), f32)
    late = pltpu.VMEM((m // 2, BK), f32)
    dma, regular = pltpu.SemaphoreType.DMA, pltpu.SemaphoreType.REGULAR
    four, items, ends = dma((4,)), dma((ITEMS,)), dma((ITEMS - 1 + SPLIT,))
    return pl.pallas_call(
        kernel,
        out_shape=jax.ShapeDtypeStruct((m, BK), f32),
        in_specs=[pl.BlockSpec(memory_space=pltpu.HBM)] * 2,
        out_specs=pl.BlockSpec(memory_space=pl.ANY),
        scratch_shapes=[
            whole, pltpu.VMEM((2, BK, BK), f32), whole, whole, whole, whole, pltpu.VMEM((m, 8 * BK), bf16), block, block, block, block,
            pltpu.VMEM((QUARTERS, 4, 4, QUARTER, BK), f32), pltpu.VMEM((QUARTERS, 8 * BK, 2 * BK), bf16), whole,
            both, both, both, both, late, late, late, late, whole, whole, whole, whole, whole,
            dma((2,)), dma, regular, regular, dma, dma, four, four, four,
            dma, dma, dma, dma, four, four, four, dma, four,
            dma, dma, items, dma, dma, items, dma, ends, dma, ends, dma, dma((PIECES + SPLIT,)),
        ],
        compiler_params=pltpu.CompilerParams(collective_id=0, has_side_effects=True, vmem_limit_bytes=52 * 2**20),
        name="panels_by_vectors",
    )(panels, eigvecs.reshape(2, BK, BK))


def solution(mesh):
    in_specs = (P("row", ("layer", "col")), P(("layer", "row"), "col"))
    return jax.shard_map(local, mesh=mesh, in_specs=in_specs, out_specs=P("row", "col"), check_vma=False)
```

```python
import jax
import jax.numpy as jnp
from jax import lax
from jax.experimental import pallas as pl
from jax.experimental.pallas import tpu as pltpu
from jax.sharding import PartitionSpec as P

MESH = pl.DeviceIdType.MESH
BK = 128
QUARTERS = 4
QUARTER = BK // QUARTERS
PIECES = 4
ITEMS = QUARTERS * PIECES
RING = 8
SPLIT = 4
LAGS = (3, 6, 7, 10)
SLOWER = {"pass_on": (8,), "close_layer": (8, 10)}


def remote(src, dst, send, recv, device):
    return pltpu.make_async_remote_copy(src_ref=src, dst_ref=dst, send_sem=send, recv_sem=recv, device_id=device, device_id_type=MESH)


def drain(ref, sem):
    pltpu.make_async_copy(ref, ref, sem).wait()


def parts(x):
    hi = x.astype(jnp.bfloat16)
    return hi, (x - hi.astype(jnp.float32)).astype(jnp.bfloat16)


def swap(a, b, width):
    even = lax.rem(lax.div(lax.broadcasted_iota(jnp.int32, a.shape, 1), width), 2) == 0
    return jnp.where(even, a, pltpu.roll(b, width, 1)), jnp.where(even, pltpu.roll(a, BK - width, 1), b)


def turn(x):
    a, b = swap(x[0], x[2], 2 * QUARTER)
    c, d = swap(x[1], x[3], 2 * QUARTER)
    return (*swap(a, c, QUARTER), *swap(b, d, QUARTER))


def kernel(
    a_hbm, e_hbm, o_hbm,
    a_ref, e_ref, o_ref, a_low, a_high, a_far, a_cat, b_mine, b_first, b_second, b_far, b_all, b_cat, keep,
    go_up, go_down, in_up, in_down, late_up, late_down, end_up, end_down, z_mine, z_in, z_pair, z_other, z_sum,
    in_sems, out_sem, plane_sem, z_sem, as_near, as_far, ar_low, ar_high, ar_far,
    bs_lead, bs_first, bs_second, bs_far, br_first, br_second, br_far, bs_plane, br_plane,
    ps_up, ps_down, pr, qs_up, qs_down, qr, zs_in, zr_in, zs_pair, zr_pair, zs_out, zr_out,
):
    layer, row, col = lax.axis_index("layer"), lax.axis_index("row"), lax.axis_index("col")
    zh, core = lax.div(row, 2), lax.rem(row, 2)
    y, x = lax.div(col, 4), lax.rem(col, 4)
    ga = x + core * (y - x)
    gb = y + core * (x - y)

    def at(a, b):
        return {"col": (1 - core) * (b * 4 + a) + core * (a * 4 + b)}

    a_up, a_down = at(lax.rem(ga + 1, 4), gb), at(lax.rem(ga + 3, 4), gb)
    b_up, b_down = at(ga, lax.rem(gb + 1, 4)), at(ga, lax.rem(gb + 3, 4))
    step = 1 - 2 * core
    zh_first, zh_second = lax.rem(zh + step + 4, 4), lax.rem(zh - step + 4, 4)
    z_first, z_second = {"row": zh_first * 2 + core}, {"row": zh_second * 2 + core}
    outer = jnp.logical_or(layer == 0, layer == 3)
    inner = jnp.logical_not(outer)
    z_inner = 1 + lax.div(layer, 2)
    z_partner = lax.rem(3 - layer, 4)
    z_outer = lax.rem(3 * layer + 1, 4)
    early = zh < 2
    lead = early.astype(jnp.int32)

    load_e = pltpu.make_async_copy(e_hbm, e_ref, in_sems.at[0])
    load_a = pltpu.make_async_copy(a_hbm, a_ref, in_sems.at[1])
    load_e.start()
    load_a.start()

    barrier = pltpu.get_barrier_semaphore()

    def greet(device):
        pl.semaphore_signal(barrier, inc=1, device_id=device, device_id_type=MESH)

    core0, core1 = zh * 2, zh * 2 + 1
    def greet_z(there, layers):
        greet({"row": there * 2, **layers})
        pl.when(there >= 2)(lambda: greet({"row": there * 2 + 1, **layers}))

    for d in (1, 3):
        greet_z(lax.rem(zh + d, 4), {})

    @pl.when(outer)
    def _():
        greet_z(zh, {"layer": z_inner})

    @pl.when(inner)
    def _():
        greet_z(zh, {"layer": z_partner})
        greet_z(zh, {"layer": z_outer})

    for d in (1, 3, 2):
        greet({"row": core1, "col": y * 4 + lax.rem(x + d, 4)})
        greet({"row": core1, "col": lax.rem(y + d, 4) * 4 + x})

    @pl.when(core == 0)
    def _():
        greet({"row": core1})

    @pl.when(core == 1)
    def _():
        greet({"row": core0})

    load_e.wait()
    for h in range(2):
        for q, packed in enumerate(turn([e_ref[h, pl.ds(g * QUARTER, QUARTER), :] for g in range(4)])):
            b_mine[q, h] = packed

    with jax.named_scope("plane_barrier"):
        @pl.when(core == 1)
        def _():
            pl.semaphore_wait(barrier, 13 + (1 - lead) * (6 + 2 * inner.astype(jnp.int32)))
            pl.semaphore_signal(plane_sem, inc=1, device_id={"row": core0}, device_id_type=MESH)

        @pl.when(core == 0)
        def _():
            pl.semaphore_wait(plane_sem, 1)

    rows = [pl.ds(p * (a_ref.shape[0] // PIECES), a_ref.shape[0] // PIECES) for p in range(PIECES)]
    ups = [remote(a_ref.at[r], a_low.at[r], as_near, ar_low.at[p], a_up) for p, r in enumerate(rows)]
    downs = [remote(a_ref.at[r], a_high.at[r], as_near, ar_high.at[p], a_down) for p, r in enumerate(rows)]
    a_fars = [
        remote(a_high.at[r], a_far.at[r], as_far, ar_far.at[p], a_down) if p % 2
        else remote(a_low.at[r], a_far.at[r], as_far, ar_far.at[p], a_up)
        for p, r in enumerate(rows)
    ]

    def send_piece(p):
        ups[p].start()
        downs[p].start()

    def relay(p):
        with jax.named_scope(f"relay{p}"):
            (downs if p % 2 else ups)[p].wait_recv()
        a_fars[p].start()

    firsts = [remote(b_mine.at[q], b_first.at[q], bs_first if q else bs_lead, br_first.at[q], z_first) for q in range(QUARTERS)]
    seconds = [remote(b_mine.at[q], b_second.at[q], bs_second, br_second.at[q], z_second) for q in range(QUARTERS)]
    b_fars = [remote(b_first.at[q], b_far.at[q], bs_far, br_far.at[q], z_first) for q in range(QUARTERS)]
    blocks = ((b_mine, zh), (b_first, zh_second), (b_second, zh_first), (b_far, lax.rem(zh + 2, 4)))

    def exchange(q, k):
        held, source = blocks[k]
        src = held.at[q]
        copies = [(jnp.logical_and(core == 0, source == y), src, b_all.at[q, pl.ds(2 * core, 2), y], {"row": core0, "col": source * 4 + x})]
        for h in range(2):
            copies.append((
                jnp.logical_and(core == 1, x == 2 * core + h), src.at[h], b_all.at[q, source, x], {"row": core1, "col": y * 4 + 2 * core + h},
            ))
        for own, src, dst, device in copies:
            @pl.when(own)
            def _():
                pltpu.make_async_copy(src, dst, br_plane.at[q]).start()

            @pl.when(jnp.logical_not(own))
            def _():
                remote(src, dst, bs_plane, br_plane.at[q], device).start()

    def arrived(copies, q):
        name = "b_first" if copies is firsts else "b_second" if copies is seconds else "b_far"
        with jax.named_scope(f"{name}{q}"):
            copies[q].wait_recv()

    size = a_ref.shape[0] // ITEMS
    part = size // 2

    def span(m):
        return pl.ds(pl.multiple_of(m * size, size), size)

    def top(m):
        return pl.ds(pl.multiple_of(m * part, part), part)

    def whole(p):
        return pl.ds(pl.multiple_of(p * 4 * size, 4 * size), 4 * size)

    def take_piece(p):
        r = whole(p)
        with jax.named_scope("piece"):
            drain(a_far.at[r], ar_far.at[p])

            @pl.when(lax.rem(p, 2) == 0)
            def _():
                drain(a_high.at[r], ar_high.at[p])

            @pl.when(lax.rem(p, 2) == 1)
            def _():
                drain(a_low.at[r], ar_low.at[p])

        for i, ref in enumerate((a_ref, a_high, a_far, a_low)):
            hi, lo = parts(ref[r, :])
            a_cat[r, pl.ds(i * BK, BK)] = hi
            a_cat[r, pl.ds((4 + i) * BK, BK)] = lo

    exchange(0, 0)
    load_a.wait()
    send_piece(0)
    send_piece(1)

    @pl.when(zh == 0)
    def _():
        send_piece(2)
        send_piece(3)
        relay(0)

    with jax.named_scope("z_barrier"):
        @pl.when(core == 0)
        def _():
            pl.semaphore_wait(barrier, 7 + 2 * inner.astype(jnp.int32))
            pl.when(early)(lambda: pl.semaphore_signal(z_sem, inc=1, device_id={"row": core1}, device_id_type=MESH))

        @pl.when(jnp.logical_and(core == 1, early))
        def _():
            pl.semaphore_wait(z_sem, 1)

    firsts[0].start()
    with jax.named_scope("b_lead"):
        firsts[0].wait_send()
    seconds[0].start()
    firsts[1].start()

    @pl.when(zh == 1)
    def _():
        relay(0)
        send_piece(2)

    arrived(firsts, 0)
    b_fars[0].start()
    firsts[2].start()
    exchange(0, 1)
    pl.when(jnp.logical_not(early))(lambda: relay(0))
    pl.when(early)(lambda: relay(1))
    pl.when(zh == 1)(lambda: send_piece(3))
    arrived(seconds, 0)
    exchange(0, 2)
    seconds[1].start()
    arrived(firsts, 1)
    b_fars[1].start()
    pl.when(early)(lambda: relay(2))

    @pl.when(jnp.logical_not(early))
    def _():
        relay(1)
        send_piece(2)

    arrived(b_fars, 0)
    exchange(0, 3)
    firsts[3].start()
    exchange(1, 0)
    exchange(1, 1)
    take_piece(0)
    arrived(firsts, 2)
    b_fars[2].start()
    seconds[2].start()
    pl.when(early)(lambda: relay(3))

    @pl.when(jnp.logical_not(early))
    def _():
        relay(2)
        send_piece(3)

    arrived(seconds, 1)
    exchange(1, 2)
    take_piece(1)
    arrived(b_fars, 1)
    exchange(1, 3)

    def factor(q):
        with jax.named_scope(f"factor{q}"):
            drain(b_all.at[q], br_plane.at[q])
            for i in range(4):
                k = lax.rem(ga + i, 4)
                for g, block in enumerate(turn([b_all[q, k, lax.rem(gb + j, 4)] for j in range(4)])):
                    hi, lo = parts(block)
                    for r in (i * BK + g * QUARTER, 4 * BK + i * BK + g * QUARTER):
                        b_cat[q, pl.ds(r, QUARTER), pl.ds(0, BK)] = hi
                        b_cat[q, pl.ds(r, QUARTER), pl.ds(BK, BK)] = lo

    def place(t):
        b, c = lax.div(t, 9), lax.div(t, 12)
        q = (1 - b) * lax.div(t, 3) + (b - c) * (t - 9) + c * 3
        p = (1 - b) * lax.rem(t, 3) + (b - c) * 3 + c * (t - 12)
        return lead * lax.div(t, PIECES) + (1 - lead) * q, lead * lax.rem(t, PIECES) + (1 - lead) * p

    def item(q, p):
        b = lax.div(p, 3)
        return lead * (PIECES * q + p) + (1 - lead) * ((1 - b) * (3 * q + p) + b * (9 + q))

    def multiply(t):
        q, p = place(t)
        pl.when(jnp.logical_and(q == 0, p >= 2))(lambda: take_piece(p))
        out = jnp.dot(a_cat[whole(p), :], b_cat[q], preferred_element_type=jnp.float32)
        out = out[:, :BK] + out[:, BK:]
        mine, above, far, below = turn([out[g * size:(g + 1) * size] for g in range(4)])
        keep[span(t), :] = mine
        late_up[top(t), :] = above[:part]
        late_down[top(t), :] = below[part:]
        go_up[t, 0], go_up[t, 1] = far[:part], above[part:]
        go_down[t, 0], go_down[t, 1] = far[part:], below[:part]
        remote(go_up.at[t], in_up.at[t], ps_up, pr.at[lax.rem(t, RING)], b_up).start()
        remote(go_down.at[t], in_down.at[t], ps_down, pr.at[lax.rem(t, RING)], b_down).start()

    def pass_on(m):
        drain(a_ref.at[pl.ds(0, 2 * size)], pr.at[lax.rem(m, RING)])
        late_up[top(m), :] += in_up[m, 0]
        remote(late_up.at[top(m)], end_up.at[top(m)], qs_up, qr.at[lax.rem(m, RING)], b_up).start()
        late_down[top(m), :] += in_down[m, 0]
        remote(late_down.at[top(m)], end_down.at[top(m)], qs_down, qr.at[lax.rem(m, RING)], b_down).start()

    def close_layer(m):
        drain(z_mine.at[span(m)], qr.at[lax.rem(m, RING)])
        low, high = top(2 * m), top(2 * m + 1)
        z_mine[low, :] = keep[low, :] + (end_up[top(m), :] + in_down[m, 1])
        z_mine[high, :] = keep[high, :] + (in_up[m, 1] + end_down[top(m), :])

        def send(r, k):
            pl.when(outer)(lambda: remote(z_mine.at[r], z_in.at[r], zs_in, zr_in.at[k], {"layer": z_inner}).start())

        by_parts(m, send)

    def by_parts(m, act):
        pl.when(m < ITEMS - 1)(lambda: act(span(m), m))

        @pl.when(m == ITEMS - 1)
        def _():
            for i in range(SPLIT):
                act(pl.ds((ITEMS - 1) * size + i * (size // SPLIT), size // SPLIT), ITEMS - 1 + i)

    def pair_up(m):
        def act(r, k):
            drain(z_in.at[r], zr_in.at[k])
            z_pair[r, :] = z_mine[r, :] + z_in[r, :]
            remote(z_pair.at[r], z_other.at[r], zs_pair, zr_pair.at[lax.rem(k, ITEMS - 1 - RING + SPLIT)], {"layer": z_partner}).start()

        by_parts(m, act)

    def unpack(t):
        q, p = place(t)

        @pl.when(q == 3)
        def _():
            for g, block in enumerate(turn([z_sum[span(m), :] for m in [item(i, p) for i in range(QUARTERS - 1)] + [t]])):
                o_ref[span(4 * p + g), :] = block
            pltpu.make_async_copy(o_ref.at[whole(p)], o_hbm.at[whole(p)], out_sem).start()

    def last(k):
        return (k - ITEMS + PIECES + 1) * lax.div(k, ITEMS - PIECES)

    def finish(m):
        def act(r, k):
            drain(z_other.at[r], zr_pair.at[lax.rem(k, ITEMS - 1 - RING + SPLIT)])
            z_sum[r, :] = z_pair[r, :] + z_other[r, :]
            remote(z_sum.at[r], z_sum.at[r], zs_out, zr_out.at[last(k)], {"layer": z_outer}).start()

        by_parts(m, act)
        unpack(m)

    def run(stage, m):
        jax.named_scope(stage.__name__)(stage)(m)

    factor(0)
    lax.fori_loop(0, 2, lambda t, carry: (run(multiply, t), carry)[1], 0)

    exchange(2, 0)
    exchange(2, 1)
    arrived(seconds, 2)
    exchange(2, 2)
    arrived(firsts, 3)
    b_fars[3].start()
    seconds[3].start()
    pl.when(jnp.logical_not(early))(lambda: run(pass_on, 0))
    run(multiply, 2)
    pl.when(early)(lambda: run(pass_on, 0))
    pl.when(jnp.logical_not(early))(lambda: relay(3))
    arrived(b_fars, 2)
    exchange(2, 3)
    pl.when(jnp.logical_not(early))(lambda: factor(1))
    run(multiply, 3)
    run(pass_on, 1)
    stages = tuple(zip((multiply, pass_on, close_layer, pair_up, finish), (0, *LAGS), (4, 2, 0, 0, 0), (None, None, None, inner, inner)))

    def body(t, carry):
        pl.when(jnp.logical_and(early, t == 4))(lambda: factor(1))
        pl.when(t == 6 + 2 * lead)(lambda: factor(2))

        @pl.when(t == 5)
        def _():
            exchange(3, 0)
            exchange(3, 1)

        @pl.when(t == 6)
        def _():
            arrived(seconds, 3)
            exchange(3, 2)

        @pl.when(t == 7)
        def _():
            arrived(b_fars, 3)
            exchange(3, 3)

        pl.when(t == 12)(lambda: factor(3))
        for stage, lag, least, cond in stages:
            m = t - lag
            ok = t >= 0
            for turn_at in SLOWER.get(stage.__name__, ()):
                m += (t < turn_at).astype(jnp.int32)
                ok = jnp.logical_and(ok, t != turn_at)
            ok = jnp.logical_and(ok, jnp.logical_and(m >= least, m < ITEMS))
            if cond is not None:
                ok = jnp.logical_and(ok, cond)
            pl.when(ok)(lambda stage=stage, m=m: run(stage, m))
        return carry

    lax.fori_loop(4, ITEMS + LAGS[-1], body, 0)

    with jax.named_scope("outs"):
        @pl.when(outer)
        def _():
            def take(m, carry):
                by_parts(m, lambda r, k: drain(z_sum.at[r], zr_out.at[last(k)]))
                unpack(m)
                return carry

            drain(z_sum.at[pl.ds(0, (ITEMS - PIECES) * size)], zr_out.at[0])
            lax.fori_loop(ITEMS - PIECES, ITEMS, take, 0)
            drain(z_mine, zs_in)

        @pl.when(inner)
        def _():
            drain(z_pair, zs_pair)
            drain(z_sum, zs_out)

    with jax.named_scope("sends"):
        for ref, sem in ((go_up, ps_up), (go_down, ps_down), (late_up, qs_up), (late_down, qs_down)):
            drain(ref, sem)
        drain(a_ref, as_near)
        drain(a_ref, as_near)
        drain(a_far, as_far)
        drain(b_mine.at[pl.ds(1, 3)], bs_first)
        drain(b_mine, bs_second)
        drain(b_first, bs_far)
        for own, sent in ((core == 0, 14), (jnp.logical_and(core == 1, x < 2), 16), (jnp.logical_and(core == 1, x >= 2), 12)):
            pl.when(own)(lambda sent=sent: drain(a_ref.at[pl.ds(0, sent * BK)], bs_plane))
        pltpu.make_async_copy(o_ref, o_hbm, out_sem).wait()


def local(panels, eigvecs):
    m, f32, bf16 = panels.shape[0], jnp.float32, jnp.bfloat16
    whole = pltpu.VMEM((m, BK), f32)
    block = pltpu.VMEM((QUARTERS, 2, QUARTER, BK), f32)
    both = pltpu.VMEM((ITEMS, 2, m // ITEMS // 2, BK), f32)
    late = pltpu.VMEM((m // 2, BK), f32)
    dma, regular = pltpu.SemaphoreType.DMA, pltpu.SemaphoreType.REGULAR
    four, ring, ends = dma((4,)), dma((RING,)), dma((ITEMS - 1 + SPLIT,))
    return pl.pallas_call(
        kernel,
        out_shape=jax.ShapeDtypeStruct((m, BK), f32),
        in_specs=[pl.BlockSpec(memory_space=pltpu.HBM)] * 2,
        out_specs=pl.BlockSpec(memory_space=pl.ANY),
        scratch_shapes=[
            whole, pltpu.VMEM((2, BK, BK), f32), whole, whole, whole, whole, pltpu.VMEM((m, 8 * BK), bf16), block, block, block, block,
            pltpu.VMEM((QUARTERS, 4, 4, QUARTER, BK), f32), pltpu.VMEM((QUARTERS, 8 * BK, 2 * BK), bf16), whole,
            both, both, both, both, late, late, late, late, whole, whole, whole, whole, whole,
            dma((2,)), dma, regular, regular, dma, dma, four, four, four,
            dma, dma, dma, dma, four, four, four, dma, four,
            dma, dma, ring, dma, dma, ring, dma, ends, dma, dma((ITEMS - 1 - RING + SPLIT,)), dma, dma((PIECES + SPLIT,)),
        ],
        compiler_params=pltpu.CompilerParams(collective_id=0, has_side_effects=True, vmem_limit_bytes=52 * 2**20),
        name="panels_by_vectors",
    )(panels, eigvecs.reshape(2, BK, BK))


def solution(mesh):
    in_specs = (P("row", ("layer", "col")), P(("layer", "row"), "col"))
    return jax.shard_map(local, mesh=mesh, in_specs=in_specs, out_specs=P("row", "col"), check_vma=False)
```

```python
import jax
import jax.numpy as jnp
from jax import lax
from jax.experimental import pallas as pl
from jax.experimental.pallas import tpu as pltpu
from jax.sharding import PartitionSpec as P

MESH = pl.DeviceIdType.MESH
BK = 128
QUARTERS = 4
QUARTER = BK // QUARTERS
PIECES = 4
ITEMS = QUARTERS * PIECES
RING = 8
SPLIT = 4
LAGS = (3, 6, 7, 10)
SLOWER = {"pass_on": (8,), "close_layer": (8, 10)}


def remote(src, dst, send, recv, device):
    return pltpu.make_async_remote_copy(src_ref=src, dst_ref=dst, send_sem=send, recv_sem=recv, device_id=device, device_id_type=MESH)


def drain(ref, sem):
    pltpu.make_async_copy(ref, ref, sem).wait()


def parts(x):
    hi = x.astype(jnp.bfloat16)
    return hi, (x - hi.astype(jnp.float32)).astype(jnp.bfloat16)


def swap(a, b, width):
    even = lax.rem(lax.div(lax.broadcasted_iota(jnp.int32, a.shape, 1), width), 2) == 0
    return jnp.where(even, a, pltpu.roll(b, width, 1)), jnp.where(even, pltpu.roll(a, BK - width, 1), b)


def turn(x):
    a, b = swap(x[0], x[2], 2 * QUARTER)
    c, d = swap(x[1], x[3], 2 * QUARTER)
    return (*swap(a, c, QUARTER), *swap(b, d, QUARTER))


def kernel(
    a_hbm, e_hbm, o_hbm,
    a_ref, e_ref, o_ref, a_low, a_high, a_far, a_cat, b_mine, b_first, b_second, b_far, b_all, b_cat, keep,
    go_up, go_down, in_up, in_down, late_up, late_down, end_up, end_down, z_mine, z_in, z_pair, z_other, z_sum,
    in_sems, out_sem, plane_sem, z_sem, as_near, as_far, ar_low, ar_high, ar_far,
    bs_lead, bs_first, bs_second, bs_far, br_first, br_second, br_far, bs_plane, br_plane,
    ps_up, ps_down, pr, qs_up, qs_down, qr, zs_in, zr_in, zs_pair, zr_pair, zs_out, zr_out,
):
    layer, row, col = lax.axis_index("layer"), lax.axis_index("row"), lax.axis_index("col")
    zh, core = lax.div(row, 2), lax.rem(row, 2)
    y, x = lax.div(col, 4), lax.rem(col, 4)
    ga = x + core * (y - x)
    gb = y + core * (x - y)

    def at(a, b):
        return {"col": (1 - core) * (b * 4 + a) + core * (a * 4 + b)}

    a_up, a_down = at(lax.rem(ga + 1, 4), gb), at(lax.rem(ga + 3, 4), gb)
    b_up, b_down = at(ga, lax.rem(gb + 1, 4)), at(ga, lax.rem(gb + 3, 4))
    step = 1 - 2 * core
    zh_first, zh_second = lax.rem(zh + step + 4, 4), lax.rem(zh - step + 4, 4)
    z_first, z_second = {"row": zh_first * 2 + core}, {"row": zh_second * 2 + core}
    outer = jnp.logical_or(layer == 0, layer == 3)
    inner = jnp.logical_not(outer)
    z_inner = 1 + lax.div(layer, 2)
    z_partner = lax.rem(3 - layer, 4)
    z_outer = lax.rem(3 * layer + 1, 4)
    early = zh < 2
    lead = early.astype(jnp.int32)

    load_e = pltpu.make_async_copy(e_hbm, e_ref, in_sems.at[0])
    load_a = pltpu.make_async_copy(a_hbm, a_ref, in_sems.at[1])
    load_e.start()
    load_a.start()

    barrier = pltpu.get_barrier_semaphore()

    def greet(device):
        pl.semaphore_signal(barrier, inc=1, device_id=device, device_id_type=MESH)

    core0, core1 = zh * 2, zh * 2 + 1
    def greet_z(there, layers):
        greet({"row": there * 2, **layers})
        pl.when(there >= 2)(lambda: greet({"row": there * 2 + 1, **layers}))

    for d in (1, 3):
        greet_z(lax.rem(zh + d, 4), {})

    @pl.when(outer)
    def _():
        greet_z(zh, {"layer": z_inner})

    @pl.when(inner)
    def _():
        greet_z(zh, {"layer": z_partner})
        greet_z(zh, {"layer": z_outer})

    for d in (1, 3, 2):
        greet({"row": core1, "col": y * 4 + lax.rem(x + d, 4)})
        greet({"row": core1, "col": lax.rem(y + d, 4) * 4 + x})

    @pl.when(core == 0)
    def _():
        greet({"row": core1})

    @pl.when(core == 1)
    def _():
        greet({"row": core0})

    load_e.wait()
    for h in range(2):
        for q, packed in enumerate(turn([e_ref[h, pl.ds(g * QUARTER, QUARTER), :] for g in range(4)])):
            b_mine[q, h] = packed

    with jax.named_scope("plane_barrier"):
        @pl.when(core == 1)
        def _():
            pl.semaphore_wait(barrier, 13 + (1 - lead) * (6 + 2 * inner.astype(jnp.int32)))
            pl.semaphore_signal(plane_sem, inc=1, device_id={"row": core0}, device_id_type=MESH)

        @pl.when(core == 0)
        def _():
            pl.semaphore_wait(plane_sem, 1)

    rows = [pl.ds(p * (a_ref.shape[0] // PIECES), a_ref.shape[0] // PIECES) for p in range(PIECES)]
    ups = [remote(a_ref.at[r], a_low.at[r], as_near, ar_low.at[p], a_up) for p, r in enumerate(rows)]
    downs = [remote(a_ref.at[r], a_high.at[r], as_near, ar_high.at[p], a_down) for p, r in enumerate(rows)]
    a_fars = [
        remote(a_high.at[r], a_far.at[r], as_far, ar_far.at[p], a_down) if p % 2
        else remote(a_low.at[r], a_far.at[r], as_far, ar_far.at[p], a_up)
        for p, r in enumerate(rows)
    ]

    def send_piece(p):
        ups[p].start()
        downs[p].start()

    def relay(p):
        with jax.named_scope(f"relay{p}"):
            (downs if p % 2 else ups)[p].wait_recv()
        a_fars[p].start()

    firsts = [remote(b_mine.at[q], b_first.at[q], bs_first if q else bs_lead, br_first.at[q], z_first) for q in range(QUARTERS)]
    seconds = [remote(b_mine.at[q], b_second.at[q], bs_second, br_second.at[q], z_second) for q in range(QUARTERS)]
    b_fars = [remote(b_first.at[q], b_far.at[q], bs_far, br_far.at[q], z_first) for q in range(QUARTERS)]
    blocks = ((b_mine, zh), (b_first, zh_second), (b_second, zh_first), (b_far, lax.rem(zh + 2, 4)))

    def exchange(q, k):
        held, source = blocks[k]
        src = held.at[q]
        copies = [(jnp.logical_and(core == 0, source == y), src, b_all.at[q, pl.ds(2 * core, 2), y], {"row": core0, "col": source * 4 + x})]
        for h in range(2):
            copies.append((
                jnp.logical_and(core == 1, x == 2 * core + h), src.at[h], b_all.at[q, source, x], {"row": core1, "col": y * 4 + 2 * core + h},
            ))
        for own, src, dst, device in copies:
            @pl.when(own)
            def _():
                pltpu.make_async_copy(src, dst, br_plane.at[q]).start()

            @pl.when(jnp.logical_not(own))
            def _():
                remote(src, dst, bs_plane, br_plane.at[q], device).start()

    def arrived(copies, q):
        name = "b_first" if copies is firsts else "b_second" if copies is seconds else "b_far"
        with jax.named_scope(f"{name}{q}"):
            copies[q].wait_recv()

    size = a_ref.shape[0] // ITEMS
    part = size // 2

    def span(m):
        return pl.ds(pl.multiple_of(m * size, size), size)

    def top(m):
        return pl.ds(pl.multiple_of(m * part, part), part)

    def whole(p):
        return pl.ds(pl.multiple_of(p * 4 * size, 4 * size), 4 * size)

    def take_piece(p):
        r = whole(p)
        with jax.named_scope("piece"):
            drain(a_far.at[r], ar_far.at[p])

            @pl.when(lax.rem(p, 2) == 0)
            def _():
                drain(a_high.at[r], ar_high.at[p])

            @pl.when(lax.rem(p, 2) == 1)
            def _():
                drain(a_low.at[r], ar_low.at[p])

        for i, ref in enumerate((a_ref, a_high, a_far, a_low)):
            hi, lo = parts(ref[r, :])
            a_cat[r, pl.ds(i * BK, BK)] = hi
            a_cat[r, pl.ds((4 + i) * BK, BK)] = lo

    exchange(0, 0)
    load_a.wait()
    send_piece(0)
    send_piece(1)

    @pl.when(zh == 0)
    def _():
        for q in range(1, QUARTERS):
            exchange(q, 0)
        send_piece(2)
        send_piece(3)
        relay(0)

    with jax.named_scope("z_barrier"):
        @pl.when(core == 0)
        def _():
            pl.semaphore_wait(barrier, 7 + 2 * inner.astype(jnp.int32))
            pl.when(early)(lambda: pl.semaphore_signal(z_sem, inc=1, device_id={"row": core1}, device_id_type=MESH))

        @pl.when(jnp.logical_and(core == 1, early))
        def _():
            pl.semaphore_wait(z_sem, 1)

    firsts[0].start()
    with jax.named_scope("b_lead"):
        firsts[0].wait_send()
    seconds[0].start()
    firsts[1].start()

    @pl.when(zh == 1)
    def _():
        relay(0)
        send_piece(2)

    arrived(firsts, 0)
    b_fars[0].start()
    firsts[2].start()
    exchange(0, 1)
    pl.when(jnp.logical_not(early))(lambda: relay(0))
    pl.when(early)(lambda: relay(1))
    pl.when(zh == 1)(lambda: send_piece(3))
    arrived(seconds, 0)
    exchange(0, 2)
    seconds[1].start()
    arrived(firsts, 1)
    b_fars[1].start()
    pl.when(early)(lambda: relay(2))

    @pl.when(jnp.logical_not(early))
    def _():
        relay(1)
        send_piece(2)

    arrived(b_fars, 0)
    exchange(0, 3)
    firsts[3].start()
    pl.when(zh != 0)(lambda: exchange(1, 0))
    exchange(1, 1)
    take_piece(0)
    arrived(firsts, 2)
    b_fars[2].start()
    seconds[2].start()
    pl.when(early)(lambda: relay(3))

    @pl.when(jnp.logical_not(early))
    def _():
        relay(2)
        send_piece(3)

    arrived(seconds, 1)
    exchange(1, 2)
    take_piece(1)
    arrived(b_fars, 1)
    exchange(1, 3)

    def factor(q):
        with jax.named_scope(f"factor{q}"):
            drain(b_all.at[q], br_plane.at[q])
            for i in range(4):
                k = lax.rem(ga + i, 4)
                for g, block in enumerate(turn([b_all[q, k, lax.rem(gb + j, 4)] for j in range(4)])):
                    hi, lo = parts(block)
                    for r in (i * BK + g * QUARTER, 4 * BK + i * BK + g * QUARTER):
                        b_cat[q, pl.ds(r, QUARTER), pl.ds(0, BK)] = hi
                        b_cat[q, pl.ds(r, QUARTER), pl.ds(BK, BK)] = lo

    def place(t):
        b, c = lax.div(t, 9), lax.div(t, 12)
        q = (1 - b) * lax.div(t, 3) + (b - c) * (t - 9) + c * 3
        p = (1 - b) * lax.rem(t, 3) + (b - c) * 3 + c * (t - 12)
        return lead * lax.div(t, PIECES) + (1 - lead) * q, lead * lax.rem(t, PIECES) + (1 - lead) * p

    def item(q, p):
        b = lax.div(p, 3)
        return lead * (PIECES * q + p) + (1 - lead) * ((1 - b) * (3 * q + p) + b * (9 + q))

    def multiply(t):
        q, p = place(t)
        pl.when(jnp.logical_and(q == 0, p >= 2))(lambda: take_piece(p))
        out = jnp.dot(a_cat[whole(p), :], b_cat[q], preferred_element_type=jnp.float32)
        out = out[:, :BK] + out[:, BK:]
        mine, above, far, below = turn([out[g * size:(g + 1) * size] for g in range(4)])
        keep[span(t), :] = mine
        late_up[top(t), :] = above[:part]
        late_down[top(t), :] = below[part:]
        go_up[t, 0], go_up[t, 1] = far[:part], above[part:]
        go_down[t, 0], go_down[t, 1] = far[part:], below[:part]
        remote(go_up.at[t], in_up.at[t], ps_up, pr.at[lax.rem(t, RING)], b_up).start()
        remote(go_down.at[t], in_down.at[t], ps_down, pr.at[lax.rem(t, RING)], b_down).start()

    def pass_on(m):
        drain(a_ref.at[pl.ds(0, 2 * size)], pr.at[lax.rem(m, RING)])
        late_up[top(m), :] += in_up[m, 0]
        remote(late_up.at[top(m)], end_up.at[top(m)], qs_up, qr.at[lax.rem(m, RING)], b_up).start()
        late_down[top(m), :] += in_down[m, 0]
        remote(late_down.at[top(m)], end_down.at[top(m)], qs_down, qr.at[lax.rem(m, RING)], b_down).start()

    def close_layer(m):
        drain(z_mine.at[span(m)], qr.at[lax.rem(m, RING)])
        low, high = top(2 * m), top(2 * m + 1)
        z_mine[low, :] = keep[low, :] + (end_up[top(m), :] + in_down[m, 1])
        z_mine[high, :] = keep[high, :] + (in_up[m, 1] + end_down[top(m), :])

        def send(r, k):
            pl.when(outer)(lambda: remote(z_mine.at[r], z_in.at[r], zs_in, zr_in.at[k], {"layer": z_inner}).start())

        by_parts(m, send)

    def by_parts(m, act):
        pl.when(m < ITEMS - 1)(lambda: act(span(m), m))

        @pl.when(m == ITEMS - 1)
        def _():
            for i in range(SPLIT):
                act(pl.ds((ITEMS - 1) * size + i * (size // SPLIT), size // SPLIT), ITEMS - 1 + i)

    def pair_up(m):
        def act(r, k):
            drain(z_in.at[r], zr_in.at[k])
            z_pair[r, :] = z_mine[r, :] + z_in[r, :]
            remote(z_pair.at[r], z_other.at[r], zs_pair, zr_pair.at[lax.rem(k, ITEMS - 1 - RING + SPLIT)], {"layer": z_partner}).start()

        by_parts(m, act)

    def unpack(t):
        q, p = place(t)

        @pl.when(q == 3)
        def _():
            for g, block in enumerate(turn([z_sum[span(m), :] for m in [item(i, p) for i in range(QUARTERS - 1)] + [t]])):
                o_ref[span(4 * p + g), :] = block
            pltpu.make_async_copy(o_ref.at[whole(p)], o_hbm.at[whole(p)], out_sem).start()

    def last(k):
        return (k - ITEMS + PIECES + 1) * lax.div(k, ITEMS - PIECES)

    def finish(m):
        def act(r, k):
            drain(z_other.at[r], zr_pair.at[lax.rem(k, ITEMS - 1 - RING + SPLIT)])
            z_sum[r, :] = z_pair[r, :] + z_other[r, :]
            remote(z_sum.at[r], z_sum.at[r], zs_out, zr_out.at[last(k)], {"layer": z_outer}).start()

        by_parts(m, act)
        unpack(m)

    def run(stage, m):
        jax.named_scope(stage.__name__)(stage)(m)

    factor(0)
    lax.fori_loop(0, 2, lambda t, carry: (run(multiply, t), carry)[1], 0)

    pl.when(zh != 0)(lambda: exchange(2, 0))
    exchange(2, 1)
    arrived(seconds, 2)
    exchange(2, 2)
    arrived(firsts, 3)
    b_fars[3].start()
    seconds[3].start()
    pl.when(jnp.logical_not(early))(lambda: run(pass_on, 0))
    run(multiply, 2)
    pl.when(early)(lambda: run(pass_on, 0))
    pl.when(jnp.logical_not(early))(lambda: relay(3))
    arrived(b_fars, 2)
    exchange(2, 3)
    pl.when(jnp.logical_not(early))(lambda: factor(1))
    run(multiply, 3)
    run(pass_on, 1)
    stages = tuple(zip((multiply, pass_on, close_layer, pair_up, finish), (0, *LAGS), (4, 2, 0, 0, 0), (None, None, None, inner, inner)))

    def body(t, carry):
        pl.when(jnp.logical_and(early, t == 4))(lambda: factor(1))
        pl.when(t == 6 + 2 * lead)(lambda: factor(2))

        @pl.when(t == 5)
        def _():
            pl.when(zh != 0)(lambda: exchange(3, 0))
            exchange(3, 1)

        @pl.when(t == 6)
        def _():
            arrived(seconds, 3)
            exchange(3, 2)

        @pl.when(t == 7)
        def _():
            arrived(b_fars, 3)
            exchange(3, 3)

        pl.when(t == 12)(lambda: factor(3))
        for stage, lag, least, cond in stages:
            m = t - lag
            ok = t >= 0
            for turn_at in SLOWER.get(stage.__name__, ()):
                m += (t < turn_at).astype(jnp.int32)
                ok = jnp.logical_and(ok, t != turn_at)
            ok = jnp.logical_and(ok, jnp.logical_and(m >= least, m < ITEMS))
            if cond is not None:
                ok = jnp.logical_and(ok, cond)
            pl.when(ok)(lambda stage=stage, m=m: run(stage, m))
        return carry

    lax.fori_loop(4, ITEMS + LAGS[-1], body, 0)

    with jax.named_scope("outs"):
        @pl.when(outer)
        def _():
            def take(m, carry):
                by_parts(m, lambda r, k: drain(z_sum.at[r], zr_out.at[last(k)]))
                unpack(m)
                return carry

            drain(z_sum.at[pl.ds(0, (ITEMS - PIECES) * size)], zr_out.at[0])
            lax.fori_loop(ITEMS - PIECES, ITEMS, take, 0)
            drain(z_mine, zs_in)

        @pl.when(inner)
        def _():
            drain(z_pair, zs_pair)
            drain(z_sum, zs_out)

    with jax.named_scope("sends"):
        for ref, sem in ((go_up, ps_up), (go_down, ps_down), (late_up, qs_up), (late_down, qs_down)):
            drain(ref, sem)
        drain(a_ref, as_near)
        drain(a_ref, as_near)
        drain(a_far, as_far)
        drain(b_mine.at[pl.ds(1, 3)], bs_first)
        drain(b_mine, bs_second)
        drain(b_first, bs_far)
        for own, sent in ((core == 0, 14), (jnp.logical_and(core == 1, x < 2), 16), (jnp.logical_and(core == 1, x >= 2), 12)):
            pl.when(own)(lambda sent=sent: drain(a_ref.at[pl.ds(0, sent * BK)], bs_plane))
        pltpu.make_async_copy(o_ref, o_hbm, out_sem).wait()


def local(panels, eigvecs):
    m, f32, bf16 = panels.shape[0], jnp.float32, jnp.bfloat16
    whole = pltpu.VMEM((m, BK), f32)
    block = pltpu.VMEM((QUARTERS, 2, QUARTER, BK), f32)
    both = pltpu.VMEM((ITEMS, 2, m // ITEMS // 2, BK), f32)
    late = pltpu.VMEM((m // 2, BK), f32)
    dma, regular = pltpu.SemaphoreType.DMA, pltpu.SemaphoreType.REGULAR
    four, ring, ends = dma((4,)), dma((RING,)), dma((ITEMS - 1 + SPLIT,))
    return pl.pallas_call(
        kernel,
        out_shape=jax.ShapeDtypeStruct((m, BK), f32),
        in_specs=[pl.BlockSpec(memory_space=pltpu.HBM)] * 2,
        out_specs=pl.BlockSpec(memory_space=pl.ANY),
        scratch_shapes=[
            whole, pltpu.VMEM((2, BK, BK), f32), whole, whole, whole, whole, pltpu.VMEM((m, 8 * BK), bf16), block, block, block, block,
            pltpu.VMEM((QUARTERS, 4, 4, QUARTER, BK), f32), pltpu.VMEM((QUARTERS, 8 * BK, 2 * BK), bf16), whole,
            both, both, both, both, late, late, late, late, whole, whole, whole, whole, whole,
            dma((2,)), dma, regular, regular, dma, dma, four, four, four,
            dma, dma, dma, dma, four, four, four, dma, four,
            dma, dma, ring, dma, dma, ring, dma, ends, dma, dma((ITEMS - 1 - RING + SPLIT,)), dma, dma((PIECES + SPLIT,)),
        ],
        compiler_params=pltpu.CompilerParams(collective_id=0, has_side_effects=True, vmem_limit_bytes=52 * 2**20),
        name="panels_by_vectors",
    )(panels, eigvecs.reshape(2, BK, BK))


def solution(mesh):
    in_specs = (P("row", ("layer", "col")), P(("layer", "row"), "col"))
    return jax.shard_map(local, mesh=mesh, in_specs=in_specs, out_specs=P("row", "col"), check_vma=False)
```
